8 devices in a mesh: dp: 1 (over z), sp: 8 (over y, x, core).
Axes of the slice: x: 2, y: 2, z: 1, core: 2. Of those that a mesh axis runs over, the one named last changes fastest.
Arguments:
- hidden: bfloat16 [49152, 2048], P(('dp', 'sp'))
- tok_perm: int32 [49152], P(('dp', 'sp'))
- send_off: int32 [64], P(('dp', 'sp'))
- send_len: int32 [64], P(('dp', 'sp'))
- recv_off: int32 [64], P(('dp', 'sp'))
- recv_len: int32 [64], P(('dp', 'sp'))
- recv_doc: int32 [24576], P(('dp', 'sp'))
- recv_pos: int32 [24576], P(('dp', 'sp'))
- g_attn: bfloat16 [2048], replicated
- w_q: bfloat16 [2048, 16, 128], replicated
- w_k: bfloat16 [2048, 2, 128], replicated
- w_v: bfloat16 [2048, 2, 128], replicated
- w_o: bfloat16 [16, 128, 2048], replicated
- g_mlp: bfloat16 [2048], replicated
- w_gate: bfloat16 [2048, 11008], replicated
- w_up: bfloat16 [2048, 11008], replicated
- w_down: bfloat16 [11008, 2048], replicated
Outputs:
- output: bfloat16 [49152, 2048], P(('dp', 'sp'))
All inputs are finite; a program needn't handle non-finite values.
Results may differ from the reference program's by a relative error of at most 0.0108789.
Values are sent between devices in bfloat16 or wider.
A program may use at most 1 GiB of HBM per device.

```python
import jax
import jax.numpy as jnp
from jax import lax

GROUP_SIZE = 8
TOKENS_DEV = 6144
D = 2048
HEADS = 16
KV_HEADS = 2
HEAD = 128
FF = 11008
PIECES = 4
Q_BLOCK = 128
ROPE_BASE = 500000
RECV_CAP = TOKENS_DEV // 2
Q_PER_KV = HEADS // KV_HEADS
NORM_EPS = 1e-5


def draw_plan(plan_key):
    key_src, key_shift, key_long = jax.random.split(plan_key, 3)
    src_of = jax.vmap(lambda sub_key: jax.random.permutation(sub_key, GROUP_SIZE))(jax.random.split(key_src, PIECES)).astype(jnp.int32)
    dev_ids = jnp.arange(GROUP_SIZE, dtype=jnp.int32)
    len_shift = jax.random.randint(key_shift, (GROUP_SIZE,), 0, 6, dtype=jnp.int32)
    long_dev = jax.random.randint(key_long, (), 0, GROUP_SIZE, dtype=jnp.int32)
    len_shift = jnp.where(dev_ids == long_dev, 0, len_shift).astype(jnp.int32)
    first_len = jnp.right_shift(jnp.full((GROUP_SIZE,), RECV_CAP, jnp.int32), len_shift)
    rest_len = RECV_CAP - first_len
    piece_len = jnp.stack([first_len, rest_len // 3, (rest_len + 1) // 3, (rest_len + 2) // 3]).astype(jnp.int32)
    held_dest = jnp.argsort(src_of, axis=1).astype(jnp.int32)
    held_len = jnp.take_along_axis(piece_len, held_dest, axis=1)
    held_end = jnp.cumsum(held_len, axis=0)
    tok_idx = jnp.arange(TOKENS_DEV, dtype=jnp.int32)
    piece_idx = jnp.sum((tok_idx[None, None, :] >= held_end[:, :, None]).astype(jnp.int32), axis=0)
    dest_pad = jnp.concatenate([held_dest, jnp.full((1, GROUP_SIZE), GROUP_SIZE, jnp.int32)], axis=0)
    tok_dest = jnp.take_along_axis(dest_pad.T, piece_idx, axis=1)
    tok_perm = jnp.argsort(tok_dest * TOKENS_DEV + tok_idx[None, :], axis=1)
    to_dest = (held_dest[:, :, None] == dev_ids[None, None, :]).astype(jnp.int32)
    send_len = jnp.sum(to_dest * held_len[:, :, None], axis=0)
    send_off = jnp.cumsum(send_len, axis=1) - send_len
    recv_len = send_len.T
    recv_off = jnp.cumsum(recv_len, axis=1) - recv_len
    order_key = src_of * PIECES + jnp.arange(PIECES, dtype=jnp.int32)[:, None]
    earlier = (order_key[None, :, :] < order_key[:, None, :]).astype(jnp.int32)
    dest_start = jnp.sum(earlier * piece_len[None, :, :], axis=1)
    slot_idx = jnp.arange(RECV_CAP, dtype=jnp.int32)
    in_piece = ((slot_idx[None, None, :] >= dest_start[:, :, None]) & (slot_idx[None, None, :] < (dest_start + piece_len)[:, :, None])).astype(jnp.int32)
    recv_doc = jnp.sum(in_piece * order_key[:, :, None], axis=0)
    recv_pos = jnp.sum(in_piece * (slot_idx[None, None, :] - dest_start[:, :, None]), axis=0)
    return {
        "tok_perm": tok_perm.reshape(-1).astype(jnp.int32),
        "send_off": send_off.reshape(-1).astype(jnp.int32),
        "send_len": send_len.reshape(-1).astype(jnp.int32),
        "recv_off": recv_off.reshape(-1).astype(jnp.int32),
        "recv_len": recv_len.reshape(-1).astype(jnp.int32),
        "recv_doc": recv_doc.reshape(-1).astype(jnp.int32),
        "recv_pos": recv_pos.reshape(-1).astype(jnp.int32),
    }


def setup_inputs(seed: int = 0, part: int = 0) -> dict:
    base_key = jax.random.key(seed)
    part_key = jax.random.fold_in(base_key, part)
    key_hidden, key_plan = jax.random.split(part_key)
    weight_keys = jax.random.split(base_key, 9)
    plan_ints = draw_plan(key_plan)
    qk_std = 1.7 * D ** -0.5

    def normal_w(index, shape, std):
        return (jax.random.normal(weight_keys[index], shape, jnp.float32) * std).astype(jnp.bfloat16)

    def draw_gain(index):
        return jax.random.uniform(weight_keys[index], (D,), jnp.float32, 0.5, 1.5).astype(jnp.bfloat16)

    return {
        "hidden": jax.random.normal(key_hidden, (GROUP_SIZE * TOKENS_DEV, D), jnp.float32).astype(jnp.bfloat16),
        "tok_perm": plan_ints["tok_perm"],
        "send_off": plan_ints["send_off"],
        "send_len": plan_ints["send_len"],
        "recv_off": plan_ints["recv_off"],
        "recv_len": plan_ints["recv_len"],
        "recv_doc": plan_ints["recv_doc"],
        "recv_pos": plan_ints["recv_pos"],
        "g_attn": draw_gain(0),
        "w_q": normal_w(1, (D, HEADS, HEAD), qk_std),
        "w_k": normal_w(2, (D, KV_HEADS, HEAD), qk_std),
        "w_v": normal_w(3, (D, KV_HEADS, HEAD), D ** -0.5),
        "w_o": normal_w(4, (HEADS, HEAD, D), (HEADS * HEAD) ** -0.5),
        "g_mlp": draw_gain(5),
        "w_gate": normal_w(6, (D, FF), D ** -0.5),
        "w_up": normal_w(7, (D, FF), D ** -0.5),
        "w_down": normal_w(8, (FF, D), FF ** -0.5),
    }


def rms_norm(rows_in, gain_vec):
    rows_f = rows_in.astype(jnp.float32)
    inv_rms = lax.rsqrt(jnp.mean(rows_f * rows_f, axis=-1, keepdims=True) + NORM_EPS)
    return (rows_f * inv_rms * gain_vec.astype(jnp.float32)).astype(jnp.bfloat16)


def rope(proj, positions):
    half_dim = HEAD // 2
    inv_freq = jnp.power(jnp.float32(ROPE_BASE), -2.0 * jnp.arange(half_dim, dtype=jnp.float32) / HEAD)
    angles = positions.astype(jnp.float32)[:, None, None] * inv_freq[None, None, :]
    cos_t = jnp.cos(angles)
    sin_t = jnp.sin(angles)
    lo_half = proj[..., :half_dim]
    hi_half = proj[..., half_dim:]
    return jnp.concatenate([lo_half * cos_t - hi_half * sin_t, hi_half * cos_t + lo_half * sin_t], axis=-1)


def attend(q_rot, k_rot, v_proj, doc_ids, positions):
    k_f = k_rot.astype(jnp.float32)
    v_f = v_proj.astype(jnp.float32)
    n_blocks = RECV_CAP // Q_BLOCK

    def one_block(blk_args):
        q_blk, doc_q, pos_q = blk_args
        scores = jnp.einsum("qkgd,skd->kgqs", q_blk.astype(jnp.float32), k_f) * (HEAD ** -0.5)
        allowed = (doc_q[:, None] == doc_ids[None, :]) & (positions[None, :] <= pos_q[:, None])
        probs_bf = jax.nn.softmax(jnp.where(allowed, scores, -1e30), axis=-1).astype(jnp.bfloat16)
        return jnp.einsum("kgqs,skd->qkgd", probs_bf.astype(jnp.float32), v_f).astype(jnp.bfloat16)

    blocks_out = lax.map(one_block, (q_rot.reshape(n_blocks, Q_BLOCK, KV_HEADS, Q_PER_KV, HEAD), doc_ids.reshape(n_blocks, Q_BLOCK), positions.reshape(n_blocks, Q_BLOCK)))
    return blocks_out.reshape(RECV_CAP, HEADS * HEAD)


def layer(dest_rows, doc_ids, positions, g_attn, w_q, w_k, w_v, w_o, g_mlp, w_gate, w_up, w_down):
    normed = rms_norm(dest_rows, g_attn)
    q_proj = jnp.dot(normed, w_q.reshape(D, HEADS * HEAD), preferred_element_type=jnp.float32).reshape(RECV_CAP, HEADS, HEAD)
    k_proj = jnp.dot(normed, w_k.reshape(D, KV_HEADS * HEAD), preferred_element_type=jnp.float32).reshape(RECV_CAP, KV_HEADS, HEAD)
    v_proj = jnp.dot(normed, w_v.reshape(D, KV_HEADS * HEAD), preferred_element_type=jnp.float32).astype(jnp.bfloat16).reshape(RECV_CAP, KV_HEADS, HEAD)
    q_rot = rope(q_proj, positions).astype(jnp.bfloat16).reshape(RECV_CAP, KV_HEADS, Q_PER_KV, HEAD)
    k_rot = rope(k_proj, positions).astype(jnp.bfloat16)
    attn_heads = attend(q_rot, k_rot, v_proj, doc_ids, positions)
    attn_out = jnp.dot(attn_heads, w_o.reshape(HEADS * HEAD, D), preferred_element_type=jnp.float32).astype(jnp.bfloat16)
    resid_mid = (dest_rows.astype(jnp.float32) + attn_out.astype(jnp.float32)).astype(jnp.bfloat16)
    normed_mlp = rms_norm(resid_mid, g_mlp)
    gate_proj = jnp.dot(normed_mlp, w_gate, preferred_element_type=jnp.float32)
    up_proj = jnp.dot(normed_mlp, w_up, preferred_element_type=jnp.float32)
    hidden_act = (jax.nn.silu(gate_proj) * up_proj).astype(jnp.bfloat16)
    down_proj = jnp.dot(hidden_act, w_down, preferred_element_type=jnp.float32).astype(jnp.bfloat16)
    return (resid_mid.astype(jnp.float32) + down_proj.astype(jnp.float32)).astype(jnp.bfloat16)


def reference(hidden, tok_perm, send_off, send_len, recv_off, recv_len, recv_doc, recv_pos, g_attn, w_q, w_k, w_v, w_o, g_mlp, w_gate, w_up, w_down):
    perm_rows = tok_perm.reshape(GROUP_SIZE, TOKENS_DEV)
    send_off_m = send_off.reshape(GROUP_SIZE, GROUP_SIZE)
    send_len_m = send_len.reshape(GROUP_SIZE, GROUP_SIZE)
    recv_off_m = recv_off.reshape(GROUP_SIZE, GROUP_SIZE)
    recv_len_m = recv_len.reshape(GROUP_SIZE, GROUP_SIZE)
    doc_rows = recv_doc.reshape(GROUP_SIZE, RECV_CAP)
    pos_rows = recv_pos.reshape(GROUP_SIZE, RECV_CAP)
    dev_ids = jnp.arange(GROUP_SIZE)
    slot_idx = jnp.arange(RECV_CAP)
    sorted_idx = jnp.arange(TOKENS_DEV)

    def one_dest(dest_dev):
        run_start = recv_off_m[dest_dev]
        in_run = (slot_idx[:, None] >= run_start[None, :]) & (slot_idx[:, None] < (run_start + recv_len_m[dest_dev])[None, :])
        src_dev = jnp.clip(jnp.sum(jnp.where(in_run, dev_ids[None, :], 0), axis=1), 0, GROUP_SIZE - 1)
        src_pos = jnp.sum(jnp.where(in_run, send_off_m[:, dest_dev][None, :] + slot_idx[:, None] - run_start[None, :], 0), axis=1)
        src_pos = jnp.clip(src_pos, 0, TOKENS_DEV - 1)
        filled = jnp.any(in_run, axis=1)
        src_row = src_dev * TOKENS_DEV + perm_rows[src_dev, src_pos]
        dest_rows = jnp.where(filled[:, None], hidden[src_row], jnp.zeros((), jnp.bfloat16))
        return layer(dest_rows, doc_rows[dest_dev], pos_rows[dest_dev], g_attn, w_q, w_k, w_v, w_o, g_mlp, w_gate, w_up, w_down)

    layer_rows = lax.map(one_dest, dev_ids).reshape(GROUP_SIZE * RECV_CAP, D)

    def one_source(src_dev):
        run_start = send_off_m[src_dev]
        in_run = (sorted_idx[:, None] >= run_start[None, :]) & (sorted_idx[:, None] < (run_start + send_len_m[src_dev])[None, :])
        dest_dev = jnp.clip(jnp.sum(jnp.where(in_run, dev_ids[None, :], 0), axis=1), 0, GROUP_SIZE - 1)
        dest_slot = jnp.sum(jnp.where(in_run, recv_off_m[:, src_dev][None, :] + sorted_idx[:, None] - run_start[None, :], 0), axis=1)
        dest_slot = jnp.clip(dest_slot, 0, RECV_CAP - 1)
        was_sent = jnp.any(in_run, axis=1)
        back_rows = jnp.where(was_sent[:, None], layer_rows[dest_dev * RECV_CAP + dest_slot], jnp.zeros((), jnp.bfloat16))
        inv_perm = jnp.argsort(perm_rows[src_dev])
        return back_rows[inv_perm]

    return lax.map(one_source, dev_ids).reshape(GROUP_SIZE * TOKENS_DEV, D)
```

```python
import functools

import jax
import jax.numpy as jnp
from jax import lax
from jax.experimental import pallas as pl
from jax.experimental.layout import Layout, with_layout_constraint
from jax.experimental.pallas import tpu as pltpu
from jax.sharding import PartitionSpec as P

Q_BLOCK = 128
ROPE_BASE = 500000.0
NORM_EPS = 1e-5
NEG = -1e30
LOG2E = 1.4426950408889634

BQ = 512
BK = 512
HEAD_ROWS = 1024
LEVELS = (1024, 1536, 2048, 3072)


def row_major(x):
    return with_layout_constraint(x, Layout(major_to_minor=tuple(range(x.ndim))))


def rms_norm(rows_in, gain_vec):
    rows_f = rows_in.astype(jnp.float32)
    inv_rms = lax.rsqrt(jnp.mean(rows_f * rows_f, axis=-1, keepdims=True) + NORM_EPS)
    return (rows_f * inv_rms * gain_vec.astype(jnp.float32)).astype(jnp.bfloat16)


def rope_tables(positions, head_dim):
    half_dim = head_dim // 2
    inv_freq = jnp.power(jnp.float32(ROPE_BASE), -2.0 * jnp.arange(half_dim, dtype=jnp.float32) / head_dim)
    angles = positions.astype(jnp.float32)[:, None] * inv_freq[None, :]
    return jnp.cos(angles), jnp.sin(angles)


def rope(proj, tables):
    cos_t, sin_t = tables[0][:, None, :], tables[1][:, None, :]
    half_dim = proj.shape[-1] // 2
    lo_half = proj[..., :half_dim]
    hi_half = proj[..., half_dim:]
    return jnp.concatenate([lo_half * cos_t - hi_half * sin_t, hi_half * cos_t + lo_half * sin_t], axis=-1)


def attend_general(q_rot, k_rot, v_proj, doc_ids, positions):
    n_rows, n_kv, q_per_kv, head_dim = q_rot.shape
    n_blocks = n_rows // Q_BLOCK
    qk_scale = head_dim ** -0.5

    def one_block(blk_args):
        q_blk, doc_q, pos_q = blk_args
        scores = jnp.einsum('qkgd,skd->kgqs', q_blk, k_rot, preferred_element_type=jnp.float32) * qk_scale
        allowed = (doc_q[:, None] == doc_ids[None, :]) & (positions[None, :] <= pos_q[:, None])
        probs_bf = jax.nn.softmax(jnp.where(allowed, scores, NEG), axis=-1).astype(jnp.bfloat16)
        return jnp.einsum('kgqs,skd->qkgd', probs_bf, v_proj, preferred_element_type=jnp.float32).astype(jnp.bfloat16)

    blocks_out = lax.map(one_block, (q_rot.reshape(n_blocks, Q_BLOCK, n_kv, q_per_kv, head_dim), doc_ids.reshape(n_blocks, Q_BLOCK), positions.reshape(n_blocks, Q_BLOCK)))
    return blocks_out.reshape(n_rows, n_kv * q_per_kv * head_dim)


def qkv(rows, positions, g_attn, w_q, w_k, w_v):
    normed = rms_norm(rows, g_attn)
    tables = lax.optimization_barrier(rope_tables(positions, w_q.shape[2]))
    k_proj = jnp.einsum('td,dhe->the', normed, w_k, preferred_element_type=jnp.float32)
    v_proj = jnp.einsum('td,dhe->the', normed, w_v, preferred_element_type=jnp.float32).astype(jnp.bfloat16)
    q_proj = jnp.einsum('td,dhe->the', normed, w_q, preferred_element_type=jnp.float32)
    return rope(q_proj, tables).astype(jnp.bfloat16), rope(k_proj, tables).astype(jnp.bfloat16), v_proj


def attn_residual(rows, attn_heads, w_o):
    attn_out = jnp.dot(attn_heads, w_o.reshape(-1, rows.shape[1]), preferred_element_type=jnp.float32).astype(jnp.bfloat16)
    return (rows.astype(jnp.float32) + attn_out.astype(jnp.float32)).astype(jnp.bfloat16)


def mlp_residual(resid_mid, g_mlp, w_gate, w_up, w_down):
    normed_mlp = rms_norm(resid_mid, g_mlp)
    gate_proj = jnp.dot(normed_mlp, w_gate, preferred_element_type=jnp.float32)
    up_proj = jnp.dot(normed_mlp, w_up, preferred_element_type=jnp.float32)
    hidden_act = (jax.nn.silu(gate_proj) * up_proj).astype(jnp.bfloat16)
    down_proj = jnp.dot(hidden_act, w_down, preferred_element_type=jnp.float32).astype(jnp.bfloat16)
    return (resid_mid.astype(jnp.float32) + down_proj.astype(jnp.float32)).astype(jnp.bfloat16)


def general_path(hidden, tok_perm, send_off, send_len, recv_off, recv_len, recv_doc, recv_pos, g_attn, w_q, w_k, w_v, w_o, g_mlp, w_gate, w_up, w_down):
    n_tok, model_dim = hidden.shape
    n_cap = recv_doc.shape[0]
    group_devs = send_off.shape[0]
    zero_val = jnp.zeros((), hidden.dtype)
    pair_row = jnp.arange(n_cap)[None, :]
    dev_base = jnp.arange(group_devs)[None, :] * n_cap
    send_idx = jnp.minimum(send_off[:, None] + pair_row, n_tok - 1).reshape(-1)
    send_buf = jnp.take(hidden, jnp.take(tok_perm, send_idx), axis=0).reshape(group_devs, n_cap, model_dim)
    recv_buf = lax.all_to_all(send_buf, 'sp', 0, 0, tiled=True).reshape(group_devs * n_cap, model_dim)
    slot_idx = jnp.arange(n_cap)[:, None]
    in_run = (slot_idx >= recv_off[None, :]) & (slot_idx < (recv_off + recv_len)[None, :])
    flat_pos = jnp.sum(jnp.where(in_run, dev_base + slot_idx - recv_off[None, :], 0), axis=1)
    rows = jnp.take(recv_buf, flat_pos, axis=0)
    q_rot, k_rot, v_proj = qkv(rows, recv_pos, g_attn, w_q, w_k, w_v)
    n_kv = w_k.shape[1]
    heads = attend_general(q_rot.reshape(n_cap, n_kv, -1, w_q.shape[2]), k_rot, v_proj, recv_doc, recv_pos)
    layer_rows = mlp_residual(attn_residual(rows, heads, w_o), g_mlp, w_gate, w_up, w_down)
    back_idx = jnp.minimum(recv_off[:, None] + pair_row, n_cap - 1).reshape(-1)
    back_buf = jnp.take(layer_rows, back_idx, axis=0).reshape(group_devs, n_cap, model_dim)
    back_recv = lax.all_to_all(back_buf, 'sp', 0, 0, tiled=True).reshape(group_devs * n_cap, model_dim)
    inv_perm = jnp.argsort(tok_perm)[:, None]
    in_back = (inv_perm >= send_off[None, :]) & (inv_perm < (send_off + send_len)[None, :])
    back_pos = jnp.sum(jnp.where(in_back, dev_base + inv_perm - send_off[None, :], 0), axis=1)
    was_sent = jnp.any(in_back, axis=1)
    return jnp.where(was_sent[:, None], jnp.take(back_recv, back_pos, axis=0), zero_val)


def flash_kernel(lomin_ref, lomax_ref, lo_ref, q_ref, k_ref, v_ref, o_ref, m_ref, l_ref, acc_ref, bias_ref, *, base, shift, scale):
    qb = pl.program_id(1)
    n_heads = q_ref.shape[1] // 128
    per_part = base // BK
    q_first = base + qb * BQ
    m_ref[...] = jnp.full(m_ref.shape, NEG, jnp.float32)
    l_ref[...] = jnp.zeros(l_ref.shape, jnp.float32)
    acc_ref[...] = jnp.zeros(acc_ref.shape, jnp.float32)

    def process(kb, masked):
        k_first = kb * BK
        part = kb // per_part
        stored = part * per_part + lax.rem(kb - part * per_part + shift // BK, per_part)
        k_rows = pl.ds(pl.multiple_of(stored * BK, BK), BK)
        k_blk = k_ref[k_rows, :]
        v_blk = v_ref[k_rows, :]
        if masked:
            k_idx = k_first + lax.broadcasted_iota(jnp.int32, (BQ, BK), 1)
            q_idx = q_first + lax.broadcasted_iota(jnp.int32, (BQ, BK), 0)
            ok = (k_idx >= lo_ref[...]) & (k_idx <= q_idx)
            bias_ref[...] = jnp.where(ok, 0.0, NEG)

        def score(n):
            return lax.dot_general(q_ref[:, n * 128:(n + 1) * 128], k_blk, (((1,), (1,)), ((), ())), preferred_element_type=jnp.float32)

        s_next = score(0)
        for n in range(n_heads):
            s = s_next
            if n + 1 < n_heads:
                s_next = score(n + 1)
            if masked:
                s = s + bias_ref[...]
            m_old = m_ref[n]
            m_new = jnp.maximum(m_old, jnp.max(s, axis=1, keepdims=True))
            alpha = jnp.exp2((m_old - m_new) * scale)
            p = jnp.exp2((s - jnp.concatenate([m_new] * (BK // 128), axis=1)) * scale)
            p_sum = p[:, :128]
            for c in range(128, BK, 128):
                p_sum = p_sum + p[:, c:c + 128]
            l_ref[n] = l_ref[n] * alpha + p_sum
            m_ref[n] = m_new
            pv = jnp.dot(p.astype(jnp.bfloat16), v_blk, preferred_element_type=jnp.float32)
            acc_ref[n] = acc_ref[n] * alpha + pv

    first = lomin_ref[qb] // BK
    last = (q_first + BQ - 1) // BK
    full_from = lomax_ref[qb]

    def step(kb, carry):
        inside = (kb * BK >= full_from) & ((kb + 1) * BK - 1 <= q_first)

        @pl.when(inside)
        def _():
            process(kb, False)

        @pl.when(jnp.logical_not(inside))
        def _():
            process(kb, True)

        return carry

    lax.fori_loop(first, last + 1, step, 0)
    for n in range(n_heads):
        o_ref[:, n * 128:(n + 1) * 128] = (acc_ref[n] / jnp.sum(l_ref[n], axis=1, keepdims=True)).astype(jnp.bfloat16)


def flash(q, kv, lo, shift):
    n_rows, width = q.shape
    n_kv = kv.shape[1] // 256
    group = width // n_kv
    n_q = n_rows // BQ
    blocks = lo.reshape(n_q, BQ)
    n_h = group // 128

    def q_at(h, i, *_):
        return lax.rem(i + shift // BQ, n_q), h

    return pl.pallas_call(
        functools.partial(flash_kernel, base=n_rows, shift=shift, scale=(128 ** -0.5) * LOG2E),
        grid_spec=pltpu.PrefetchScalarGridSpec(
            num_scalar_prefetch=2,
            grid=(n_kv, n_q),
            in_specs=[
                pl.BlockSpec((BQ, 1), lambda h, i, *_: (i, 0)),
                pl.BlockSpec((BQ, group), q_at),
                pl.BlockSpec((2 * n_rows, 128), lambda h, i, *_: (0, h)),
                pl.BlockSpec((2 * n_rows, 128), lambda h, i, *_: (0, n_kv + h)),
            ],
            out_specs=pl.BlockSpec((BQ, group), q_at),
            scratch_shapes=[
                pltpu.VMEM((n_h, BQ, 128), jnp.float32),
                pltpu.VMEM((n_h, BQ, 128), jnp.float32),
                pltpu.VMEM((n_h, BQ, 128), jnp.float32),
                pltpu.VMEM((BQ, BK), jnp.float32),
            ],
        ),
        out_shape=jax.ShapeDtypeStruct((n_rows, width), jnp.bfloat16),
        compiler_params=pltpu.CompilerParams(dimension_semantics=("arbitrary", "arbitrary")),
        cost_estimate=pl.CostEstimate(flops=80_000_000_000, bytes_accessed=40_000_000, transcendentals=80_000_000),
        name="flash",
    )(jnp.min(blocks, axis=1), jnp.max(blocks, axis=1), lo[:, None], q, kv, kv)


def ring_perm(n_dev, shift):
    order = ring_order(n_dev)
    return [(order[r], order[(r + shift) % n_dev]) for r in range(n_dev)]


def ring_order(n_dev):
    return [0, 1, 2, 3, 6, 7, 4, 5]


def ring_plan(send_len_all, n_cap):
    n_dev = send_len_all.shape[0]
    totals = jnp.sum(send_len_all, axis=1)
    totals = jnp.stack([totals[d] for d in ring_order(n_dev)])
    ends = jnp.cumsum(totals)
    excess = ends - totals - n_cap * jnp.arange(n_dev, dtype=jnp.int32)
    centre = (jnp.max(excess) + jnp.min(excess)) // 2
    return totals, ends - totals, centre - excess


def balanced_path(plan, hidden, g_attn, w_q, w_k, w_v, w_o, g_mlp, w_gate, w_up, w_down):
    ext_idx, back_k, pos, n_left, n_right, bucket = plan
    n_tok, model_dim = hidden.shape
    n_cap = pos.shape[0]
    n_dev = 8
    head = HEAD_ROWS
    up, down = ring_perm(n_dev, 1), ring_perm(n_dev, -1)
    slot = jnp.arange(n_cap, dtype=jnp.int32)[:, None]
    levels = LEVELS

    def grab(idx):
        return hidden.at[idx].get(mode='promise_in_bounds')

    def exchange(cap):
        def run():
            sent = grab(jnp.concatenate([ext_idx[n_cap - cap:n_cap], ext_idx[2 * n_cap:2 * n_cap + cap]]))
            right = lax.ppermute(sent[:cap], 'sp', down)
            left = lax.ppermute(sent[cap:], 'sp', up)
            own = grab(ext_idx[n_cap:2 * n_cap])
            pad = jnp.zeros((n_cap - cap, model_dim), hidden.dtype)
            left = jnp.concatenate([left, pad], axis=0)
            right = jnp.concatenate([pad, right], axis=0)

            def pick(a, b):
                return jnp.where(slot[a:b] < n_left, left[a:b], jnp.where(slot[a:b] >= n_cap - n_right, right[a:b], own[a:b]))

            return jnp.concatenate([pick(n_cap - head, n_cap), pick(0, n_cap - head)], axis=0)
        return run

    rows = row_major(lax.switch(bucket, [exchange(cap) for cap in levels]))
    normed = row_major(rms_norm(rows, g_attn))
    tables = lax.optimization_barrier(rope_tables(jnp.roll(pos, head), w_q.shape[2]))
    n_kv, head_dim = w_k.shape[1:]
    w_kv = jnp.concatenate([w_k.reshape(model_dim, -1), w_v.reshape(model_dim, -1)], axis=1)
    kv_proj = row_major(jnp.dot(normed, w_kv, preferred_element_type=jnp.float32))
    kv_width = n_kv * head_dim

    def turn(proj):
        return rope(proj.reshape(n_cap, -1, head_dim), tables).astype(jnp.bfloat16).reshape(n_cap, -1)

    kv = row_major(jnp.concatenate([turn(kv_proj[:, :kv_width]), kv_proj[:, kv_width:].astype(jnp.bfloat16)], axis=1))
    kv_prev = lax.ppermute(kv, 'sp', up)
    q_proj = row_major(jnp.dot(normed, w_q.reshape(model_dim, -1), preferred_element_type=jnp.float32))
    q_rot = row_major(turn(q_proj))
    kv = jnp.concatenate([kv_prev, kv], axis=0)
    heads = flash(q_rot, kv, n_cap + slot[:, 0] - pos, head)
    resid_mid = row_major(attn_residual(rows, heads, w_o))
    ends = row_major(mlp_residual(resid_mid[:2 * head], g_mlp, w_gate, w_up, w_down))
    from_next = lax.ppermute(ends[head:], 'sp', down)
    from_prev = lax.ppermute(ends[:head], 'sp', up)
    resid_tail = lax.optimization_barrier((resid_mid[2 * head:], ends[:8]))[0]
    middle = row_major(mlp_residual(resid_tail, g_mlp, w_gate, w_up, w_down))

    def give_back(cap):
        extra = max(cap - head, 0)

        def run():
            parts = [ends, middle, from_next, from_prev]
            stored = lax.rem(back_k + head, n_cap)
            place = jnp.where((back_k >= 0) & (back_k < n_cap), stored, 0)
            place = jnp.where((back_k >= n_cap) & (back_k < n_cap + head), back_k, place)
            place = jnp.where((back_k < 0) & (back_k >= -head), n_cap + 2 * head + back_k, place)
            size = n_cap + 2 * head
            if extra:
                over = max(cap + head - n_cap, 0)
                n_mid = extra - over
                parts.append(lax.ppermute(jnp.concatenate([middle[:n_mid], ends[:over]], axis=0), 'sp', down))
                parts.append(lax.ppermute(jnp.concatenate([ends[2 * head - over:], middle[middle.shape[0] - n_mid:]], axis=0), 'sp', up))
                place = jnp.where((back_k >= n_cap + head) & (back_k < n_cap + cap), size + back_k - n_cap - head, place)
                place = jnp.where((back_k < -head) & (back_k >= -cap), size + 2 * extra + head + back_k, place)
                size += 2 * extra
            parts.append(jnp.zeros((16, model_dim), hidden.dtype))
            place = jnp.where((back_k < -cap) | (back_k >= n_cap + cap), size, place)
            return jnp.concatenate(parts, axis=0).at[place].get(mode='promise_in_bounds')
        return run

    return lax.switch(bucket, [give_back(cap) for cap in levels])


def solution(mesh):
    row_spec = P(('dp', 'sp'), None)
    vec_spec = P(('dp', 'sp'))
    rep_spec = P()

    def per_device(hidden, tok_perm, send_off, send_len, recv_off, recv_len, recv_doc, recv_pos, *params):
        n_tok = hidden.shape[0]
        n_cap = recv_doc.shape[0]
        n_dev = send_off.shape[0]
        at_start = jnp.arange(n_cap, dtype=jnp.int32)[None, :] == recv_off[:, None]
        start_pos = jnp.sum(jnp.where(at_start, recv_pos[None, :], 0), axis=1)
        broken = jnp.sum(jnp.where(recv_len > 0, start_pos, 0))
        mine = jnp.concatenate([recv_pos, send_len, recv_off, jnp.full((112,), broken, jnp.int32)])
        every = lax.all_gather(mine, 'sp', axis=0)
        pos_all = every[:, :n_cap]
        send_all = every[:, n_cap:n_cap + n_dev]
        roff_all = every[:, n_cap + n_dev:n_cap + 2 * n_dev]
        totals, starts, offs = ring_plan(send_all, n_cap)
        prev_totals = jnp.concatenate([totals[-1:], totals[:-1]])
        fits = jnp.all((offs >= -prev_totals) & (offs <= totals) & (jnp.abs(offs) <= n_cap))
        whole = jnp.sum(jnp.abs(every[:, n_cap + 2 * n_dev])) == 0
        use_ring = fits & whole

        me = lax.axis_index('sp').astype(jnp.int32)
        ring_at = jnp.where(me < 4, me, me ^ 2)
        after = lax.rem(ring_at + 1, n_dev)
        off = jnp.clip(offs[ring_at], -n_cap, n_cap)
        off_next = jnp.clip(offs[after], -n_cap, n_cap)
        total = totals[ring_at]
        ext_idx = lax.dynamic_slice(jnp.pad(tok_perm, (2 * n_cap, 2 * n_cap)), (n_cap + off,), (3 * n_cap,))
        n_left = jnp.maximum(-off, 0)
        n_right = jnp.maximum(off_next, 0)
        order = jnp.argsort(tok_perm)
        back_k = jnp.where(order < total, order - off, 4 * n_cap).astype(jnp.int32)
        reach = jnp.max(jnp.abs(offs))
        bucket = sum((reach > level).astype(jnp.int32) for level in LEVELS[:-1])

        order_of = ring_order(n_dev)
        runs = jnp.stack([send_all[d] for d in order_of])
        run_slot = jnp.stack([roff_all[:, d] for d in order_of])
        run_rel = starts[:, None] + jnp.cumsum(runs, axis=1) - runs - starts[ring_at] - off
        half = n_dev * n_cap // 2
        run_rel = jnp.where(run_rel >= half, run_rel - 2 * half, jnp.where(run_rel < -half, run_rel + 2 * half, run_rel))
        in_run = jnp.arange(n_cap, dtype=jnp.int32)[:, None] - run_rel.reshape(1, -1)
        run_base = (jnp.arange(n_dev, dtype=jnp.int32)[None, :] * every.shape[1] + run_slot).reshape(1, -1)
        from_at = jnp.sum(jnp.where((in_run >= 0) & (in_run < runs.reshape(1, -1)), run_base + in_run, 0), axis=1)
        pos = every.reshape(-1).at[from_at].get(mode='promise_in_bounds')

        plan = (ext_idx, back_k, pos, n_left, n_right, bucket)

        def ring(_):
            return balanced_path(plan, hidden, *params)

        def general(_):
            return general_path(hidden, tok_perm, send_off, send_len, recv_off, recv_len, recv_doc, recv_pos, *params)

        return lax.cond(use_ring, ring, general, 0)

    return jax.shard_map(per_device, mesh=mesh, in_specs=(row_spec,) + (vec_spec,) * 7 + (rep_spec,) * 9, out_specs=row_spec, check_vma=False)
```

```python
import functools

import jax
import jax.numpy as jnp
from jax import lax
from jax.experimental import pallas as pl
from jax.experimental.layout import Layout, with_layout_constraint
from jax.experimental.pallas import tpu as pltpu
from jax.sharding import PartitionSpec as P

Q_BLOCK = 128
ROPE_BASE = 500000.0
NORM_EPS = 1e-5
NEG = -1e30
LOG2E = 1.4426950408889634

BQ = 512
BK = 512
HEAD_ROWS = 1024
ROW_TILE = 512
LEVELS = (1024, 1536, 2048, 3072)


def row_major(x):
    return with_layout_constraint(x, Layout(major_to_minor=tuple(range(x.ndim))))


def rms_norm(rows_in, gain_vec):
    rows_f = rows_in.astype(jnp.float32)
    inv_rms = lax.rsqrt(jnp.mean(rows_f * rows_f, axis=-1, keepdims=True) + NORM_EPS)
    return (rows_f * inv_rms * gain_vec.astype(jnp.float32)).astype(jnp.bfloat16)


def rope_tables(positions, head_dim):
    half_dim = head_dim // 2
    inv_freq = jnp.power(jnp.float32(ROPE_BASE), -2.0 * jnp.arange(half_dim, dtype=jnp.float32) / head_dim)
    angles = positions.astype(jnp.float32)[:, None] * inv_freq[None, :]
    return jnp.cos(angles), jnp.sin(angles)


def rope(proj, tables):
    cos_t, sin_t = tables[0][:, None, :], tables[1][:, None, :]
    half_dim = proj.shape[-1] // 2
    lo_half = proj[..., :half_dim]
    hi_half = proj[..., half_dim:]
    return jnp.concatenate([lo_half * cos_t - hi_half * sin_t, hi_half * cos_t + lo_half * sin_t], axis=-1)


def attend_general(q_rot, k_rot, v_proj, doc_ids, positions):
    n_rows, n_kv, q_per_kv, head_dim = q_rot.shape
    n_blocks = n_rows // Q_BLOCK
    qk_scale = head_dim ** -0.5

    def one_block(blk_args):
        q_blk, doc_q, pos_q = blk_args
        scores = jnp.einsum('qkgd,skd->kgqs', q_blk, k_rot, preferred_element_type=jnp.float32) * qk_scale
        allowed = (doc_q[:, None] == doc_ids[None, :]) & (positions[None, :] <= pos_q[:, None])
        probs_bf = jax.nn.softmax(jnp.where(allowed, scores, NEG), axis=-1).astype(jnp.bfloat16)
        return jnp.einsum('kgqs,skd->qkgd', probs_bf, v_proj, preferred_element_type=jnp.float32).astype(jnp.bfloat16)

    blocks_out = lax.map(one_block, (q_rot.reshape(n_blocks, Q_BLOCK, n_kv, q_per_kv, head_dim), doc_ids.reshape(n_blocks, Q_BLOCK), positions.reshape(n_blocks, Q_BLOCK)))
    return blocks_out.reshape(n_rows, n_kv * q_per_kv * head_dim)


def qkv(rows, positions, g_attn, w_q, w_k, w_v):
    normed = rms_norm(rows, g_attn)
    tables = lax.optimization_barrier(rope_tables(positions, w_q.shape[2]))
    k_proj = jnp.einsum('td,dhe->the', normed, w_k, preferred_element_type=jnp.float32)
    v_proj = jnp.einsum('td,dhe->the', normed, w_v, preferred_element_type=jnp.float32).astype(jnp.bfloat16)
    q_proj = jnp.einsum('td,dhe->the', normed, w_q, preferred_element_type=jnp.float32)
    return rope(q_proj, tables).astype(jnp.bfloat16), rope(k_proj, tables).astype(jnp.bfloat16), v_proj


def attn_residual(rows, attn_heads, w_o):
    attn_out = jnp.dot(attn_heads, w_o.reshape(-1, rows.shape[1]), preferred_element_type=jnp.float32).astype(jnp.bfloat16)
    return (rows.astype(jnp.float32) + attn_out.astype(jnp.float32)).astype(jnp.bfloat16)


def mlp_residual(resid_mid, g_mlp, w_gate, w_up, w_down):
    normed_mlp = rms_norm(resid_mid, g_mlp)
    gate_proj = jnp.dot(normed_mlp, w_gate, preferred_element_type=jnp.float32)
    up_proj = jnp.dot(normed_mlp, w_up, preferred_element_type=jnp.float32)
    hidden_act = (jax.nn.silu(gate_proj) * up_proj).astype(jnp.bfloat16)
    down_proj = jnp.dot(hidden_act, w_down, preferred_element_type=jnp.float32).astype(jnp.bfloat16)
    return (resid_mid.astype(jnp.float32) + down_proj.astype(jnp.float32)).astype(jnp.bfloat16)


def general_path(hidden, tok_perm, send_off, send_len, recv_off, recv_len, recv_doc, recv_pos, g_attn, w_q, w_k, w_v, w_o, g_mlp, w_gate, w_up, w_down):
    n_tok, model_dim = hidden.shape
    n_cap = recv_doc.shape[0]
    group_devs = send_off.shape[0]
    zero_val = jnp.zeros((), hidden.dtype)
    pair_row = jnp.arange(n_cap)[None, :]
    dev_base = jnp.arange(group_devs)[None, :] * n_cap
    send_idx = jnp.minimum(send_off[:, None] + pair_row, n_tok - 1).reshape(-1)
    send_buf = jnp.take(hidden, jnp.take(tok_perm, send_idx), axis=0).reshape(group_devs, n_cap, model_dim)
    recv_buf = lax.all_to_all(send_buf, 'sp', 0, 0, tiled=True).reshape(group_devs * n_cap, model_dim)
    slot_idx = jnp.arange(n_cap)[:, None]
    in_run = (slot_idx >= recv_off[None, :]) & (slot_idx < (recv_off + recv_len)[None, :])
    flat_pos = jnp.sum(jnp.where(in_run, dev_base + slot_idx - recv_off[None, :], 0), axis=1)
    rows = jnp.take(recv_buf, flat_pos, axis=0)
    q_rot, k_rot, v_proj = qkv(rows, recv_pos, g_attn, w_q, w_k, w_v)
    n_kv = w_k.shape[1]
    heads = attend_general(q_rot.reshape(n_cap, n_kv, -1, w_q.shape[2]), k_rot, v_proj, recv_doc, recv_pos)
    layer_rows = mlp_residual(attn_residual(rows, heads, w_o), g_mlp, w_gate, w_up, w_down)
    back_idx = jnp.minimum(recv_off[:, None] + pair_row, n_cap - 1).reshape(-1)
    back_buf = jnp.take(layer_rows, back_idx, axis=0).reshape(group_devs, n_cap, model_dim)
    back_recv = lax.all_to_all(back_buf, 'sp', 0, 0, tiled=True).reshape(group_devs * n_cap, model_dim)
    inv_perm = jnp.argsort(tok_perm)[:, None]
    in_back = (inv_perm >= send_off[None, :]) & (inv_perm < (send_off + send_len)[None, :])
    back_pos = jnp.sum(jnp.where(in_back, dev_base + inv_perm - send_off[None, :], 0), axis=1)
    was_sent = jnp.any(in_back, axis=1)
    return jnp.where(was_sent[:, None], jnp.take(back_recv, back_pos, axis=0), zero_val)


def flash_kernel(lomin_ref, lomax_ref, lo_ref, q_ref, k_ref, v_ref, o_ref, m_ref, l_ref, acc_ref, bias_ref, *, base, shift, scale):
    qb = pl.program_id(1)
    n_heads = q_ref.shape[1] // 128
    per_part = base // BK
    q_first = base + qb * BQ
    m_ref[...] = jnp.full(m_ref.shape, NEG, jnp.float32)
    l_ref[...] = jnp.zeros(l_ref.shape, jnp.float32)
    acc_ref[...] = jnp.zeros(acc_ref.shape, jnp.float32)

    def process(kb, masked):
        k_first = kb * BK
        part = kb // per_part
        stored = part * per_part + lax.rem(kb - part * per_part + shift // BK, per_part)
        k_rows = pl.ds(pl.multiple_of(stored * BK, BK), BK)
        k_blk = k_ref[k_rows, :]
        v_blk = v_ref[k_rows, :]
        if masked:
            k_idx = k_first + lax.broadcasted_iota(jnp.int32, (BQ, BK), 1)
            q_idx = q_first + lax.broadcasted_iota(jnp.int32, (BQ, BK), 0)
            ok = (k_idx >= lo_ref[...]) & (k_idx <= q_idx)
            bias_ref[...] = jnp.where(ok, 0.0, NEG)

        def score(n):
            return lax.dot_general(q_ref[:, n * 128:(n + 1) * 128], k_blk, (((1,), (1,)), ((), ())), preferred_element_type=jnp.float32)

        s_next = score(0)
        for n in range(n_heads):
            s = s_next
            if n + 1 < n_heads:
                s_next = score(n + 1)
            if masked:
                s = s + bias_ref[...]
            m_old = m_ref[n]
            m_new = jnp.maximum(m_old, jnp.max(s, axis=1, keepdims=True))
            alpha = jnp.exp2((m_old - m_new) * scale)
            p = jnp.exp2((s - jnp.concatenate([m_new] * (BK // 128), axis=1)) * scale)
            p_sum = p[:, :128]
            for c in range(128, BK, 128):
                p_sum = p_sum + p[:, c:c + 128]
            l_ref[n] = l_ref[n] * alpha + p_sum
            m_ref[n] = m_new
            pv = jnp.dot(p.astype(jnp.bfloat16), v_blk, preferred_element_type=jnp.float32)
            acc_ref[n] = acc_ref[n] * alpha + pv

    first = lomin_ref[qb] // BK
    last = (q_first + BQ - 1) // BK
    full_from = lomax_ref[qb]

    def step(kb, carry):
        inside = (kb * BK >= full_from) & ((kb + 1) * BK - 1 <= q_first)

        @pl.when(inside)
        def _():
            process(kb, False)

        @pl.when(jnp.logical_not(inside))
        def _():
            process(kb, True)

        return carry

    lax.fori_loop(first, last + 1, step, 0)
    for n in range(n_heads):
        o_ref[:, n * 128:(n + 1) * 128] = (acc_ref[n] / jnp.sum(l_ref[n], axis=1, keepdims=True)).astype(jnp.bfloat16)


def flash(q, kv, lo, shift):
    n_rows, width = q.shape
    n_kv = kv.shape[1] // 256
    group = width // n_kv
    n_q = n_rows // BQ
    blocks = lo.reshape(n_q, BQ)
    n_h = group // 128

    def q_at(h, i, *_):
        return lax.rem(i + shift // BQ, n_q), h

    return pl.pallas_call(
        functools.partial(flash_kernel, base=n_rows, shift=shift, scale=(128 ** -0.5) * LOG2E),
        grid_spec=pltpu.PrefetchScalarGridSpec(
            num_scalar_prefetch=2,
            grid=(n_kv, n_q),
            in_specs=[
                pl.BlockSpec((BQ, 1), lambda h, i, *_: (i, 0)),
                pl.BlockSpec((BQ, group), q_at),
                pl.BlockSpec((2 * n_rows, 128), lambda h, i, *_: (0, h)),
                pl.BlockSpec((2 * n_rows, 128), lambda h, i, *_: (0, n_kv + h)),
            ],
            out_specs=pl.BlockSpec((BQ, group), q_at),
            scratch_shapes=[
                pltpu.VMEM((n_h, BQ, 128), jnp.float32),
                pltpu.VMEM((n_h, BQ, 128), jnp.float32),
                pltpu.VMEM((n_h, BQ, 128), jnp.float32),
                pltpu.VMEM((BQ, BK), jnp.float32),
            ],
        ),
        out_shape=jax.ShapeDtypeStruct((n_rows, width), jnp.bfloat16),
        compiler_params=pltpu.CompilerParams(dimension_semantics=("arbitrary", "arbitrary")),
        cost_estimate=pl.CostEstimate(flops=80_000_000_000, bytes_accessed=40_000_000, transcendentals=80_000_000),
        name="flash",
    )(jnp.min(blocks, axis=1), jnp.max(blocks, axis=1), lo[:, None], q, kv, kv)


def norm_block(x_ref, g_ref, rows):
    x = x_ref[rows, :].astype(jnp.float32)
    inv = lax.rsqrt(jnp.mean(x * x, axis=1, keepdims=True) + NORM_EPS)
    return (x * inv * g_ref[...].astype(jnp.float32)).astype(jnp.bfloat16)


def proj_kernel(x_ref, g_ref, cos_ref, sin_ref, w_ref, o_ref, *, turned):
    h = norm_block(x_ref, g_ref, slice(None))
    width = w_ref.shape[1]
    for c in range(0, width, 256):
        y = jnp.dot(h, w_ref[:, c:c + 256], preferred_element_type=jnp.float32)
        for e in range(0, 256, 128):
            part = y[:, e:e + 128]
            if c + e < turned:
                part = part * cos_ref[...] + pltpu.roll(part, 64, 1) * sin_ref[...]
            o_ref[:, c + e:c + e + 128] = part.astype(jnp.bfloat16)


def project(x, gain, cos2, sin2, w, turned):
    n_rows, dim = x.shape
    width = w.shape[1]
    return pl.pallas_call(
        functools.partial(proj_kernel, turned=turned),
        grid=(n_rows // ROW_TILE,),
        in_specs=[
            pl.BlockSpec((ROW_TILE, dim), lambda i: (i, 0)),
            pl.BlockSpec((1, dim), lambda i: (0, 0)),
            pl.BlockSpec((ROW_TILE, 128), lambda i: (i, 0)),
            pl.BlockSpec((ROW_TILE, 128), lambda i: (i, 0)),
            pl.BlockSpec((dim, width), lambda i: (0, 0)),
        ],
        out_specs=pl.BlockSpec((ROW_TILE, width), lambda i: (i, 0)),
        out_shape=jax.ShapeDtypeStruct((n_rows, width), jnp.bfloat16),
        compiler_params=pltpu.CompilerParams(dimension_semantics=("arbitrary",)),
        cost_estimate=pl.CostEstimate(flops=2 * n_rows * dim * width, bytes_accessed=2 * (n_rows * (dim + width) + dim * width), transcendentals=0),
        name="project",
    )(x, gain[None, :], cos2, sin2, w)


def gate_up_kernel(z_ref, g_ref, wg_ref, wu_ref, o_ref, h_ref):
    n_rows = z_ref.shape[0]

    @pl.when(pl.program_id(0) == 0)
    def _():
        for r in range(0, n_rows, 256):
            h_ref[r:r + 256, :] = norm_block(z_ref, g_ref, slice(r, r + 256))

    for r in range(0, n_rows, ROW_TILE):
        h = h_ref[r:r + ROW_TILE, :]
        gate = jnp.dot(h, wg_ref[...], preferred_element_type=jnp.float32)
        up = jnp.dot(h, wu_ref[...], preferred_element_type=jnp.float32)
        o_ref[r:r + ROW_TILE, :] = (jax.nn.silu(gate) * up).astype(jnp.bfloat16)


def gate_up(z, first, n_rows, gain, w_gate, w_up, tile=256):
    dim = z.shape[1]
    ff = w_gate.shape[1]
    return pl.pallas_call(
        gate_up_kernel,
        grid=(ff // tile,),
        in_specs=[
            pl.BlockSpec((n_rows, dim), lambda j: (first // n_rows, 0)),
            pl.BlockSpec((1, dim), lambda j: (0, 0)),
            pl.BlockSpec((dim, tile), lambda j: (0, j)),
            pl.BlockSpec((dim, tile), lambda j: (0, j)),
        ],
        out_specs=pl.BlockSpec((n_rows, tile), lambda j: (0, j)),
        out_shape=jax.ShapeDtypeStruct((n_rows, ff), jnp.bfloat16),
        scratch_shapes=[pltpu.VMEM((n_rows, dim), jnp.bfloat16)],
        compiler_params=pltpu.CompilerParams(dimension_semantics=("arbitrary",)),
        cost_estimate=pl.CostEstimate(flops=4 * n_rows * dim * ff, bytes_accessed=2 * (n_rows * (dim + ff) + 2 * dim * ff), transcendentals=n_rows * ff),
        name="gate_up",
    )(z, gain[None, :], w_gate, w_up)


def ring_perm(n_dev, shift):
    order = ring_order(n_dev)
    return [(order[r], order[(r + shift) % n_dev]) for r in range(n_dev)]


def ring_order(n_dev):
    return [0, 1, 2, 3, 6, 7, 4, 5]


def ring_plan(send_len_all, n_cap):
    n_dev = send_len_all.shape[0]
    totals = jnp.sum(send_len_all, axis=1)
    totals = jnp.stack([totals[d] for d in ring_order(n_dev)])
    ends = jnp.cumsum(totals)
    excess = ends - totals - n_cap * jnp.arange(n_dev, dtype=jnp.int32)
    centre = (jnp.max(excess) + jnp.min(excess)) // 2
    return totals, ends - totals, centre - excess


def balanced_path(plan, hidden, tok_perm, g_attn, w_q, w_k, w_v, w_o, g_mlp, w_gate, w_up, w_down):
    ext_idx, from_at, every, off, total, n_left, n_right, bucket = plan
    model_dim = hidden.shape[1]
    n_cap = from_at.shape[0]
    n_dev = 8
    head = HEAD_ROWS
    up, down = ring_perm(n_dev, 1), ring_perm(n_dev, -1)
    slot = jnp.arange(n_cap, dtype=jnp.int32)
    levels = LEVELS
    n_kv, head_dim = w_k.shape[1:]

    def grab(idx):
        return hidden.at[idx].get(mode='promise_in_bounds')

    def exchange(cap):
        def run():
            right = lax.ppermute(grab(ext_idx[n_cap - cap:n_cap]), 'sp', down)
            left = lax.ppermute(grab(ext_idx[2 * n_cap:2 * n_cap + cap]), 'sp', up)
            rows = row_major(grab(jnp.roll(ext_idx[n_cap:2 * n_cap], head)))
            pos = every.reshape(-1).at[from_at].get(mode='promise_in_bounds')
            cos_t, sin_t = rope_tables(jnp.roll(pos, head), head_dim)
            cos2 = jnp.concatenate([cos_t, cos_t], axis=1)
            sin2 = jnp.concatenate([-sin_t, sin_t], axis=1)
            order = jnp.argsort(tok_perm)
            back_k = jnp.where(order < total, order - off, 4 * n_cap).astype(jnp.int32)
            w_kv = jnp.concatenate([w_k.reshape(model_dim, -1), w_v.reshape(model_dim, -1)], axis=1)

            def merge(rows, stored, vals, keep):
                size = vals.shape[0]
                return rows.at[stored:stored + size].set(jnp.where(keep[:, None], vals, rows[stored:stored + size]))

            step = jnp.arange(cap, dtype=jnp.int32)
            keep_l, keep_r = step < n_left, step >= cap - n_right
            cut = min(cap, n_cap - head)
            rows = merge(rows, head, left[:cut], keep_l[:cut])
            if cap > cut:
                rows = merge(rows, 0, left[cut:], keep_l[cut:])
            cut = max(cap - head, 0)
            rows = merge(rows, 0, right[cut:], keep_r[cut:])
            if cut:
                rows = merge(rows, n_cap - cut, right[:cut], keep_r[:cut])
            return rows, pos, cos2, sin2, back_k, w_q.reshape(model_dim, -1), w_kv
        return run

    rows, pos, cos2, sin2, back_k, w_q2, w_kv = lax.switch(bucket, [exchange(cap) for cap in levels])
    rows = row_major(rows)
    kv = project(rows, g_attn, cos2, sin2, w_kv, n_kv * head_dim)
    kv_prev = lax.ppermute(kv, 'sp', up)
    q_rot = project(rows, g_attn, cos2, sin2, w_q2, w_q2.shape[1])
    kv = jnp.concatenate([kv_prev, kv], axis=0)
    heads = flash(q_rot, kv, n_cap + slot - pos, head)
    resid_mid = row_major(attn_residual(rows, heads, w_o))

    def mlp(first, n_rows):
        z = resid_mid[first:first + n_rows]
        acts = gate_up(resid_mid, first, n_rows, g_mlp, w_gate, w_up)
        down_proj = jnp.dot(acts, w_down, preferred_element_type=jnp.float32).astype(jnp.bfloat16)
        return row_major((z.astype(jnp.float32) + down_proj.astype(jnp.float32)).astype(jnp.bfloat16))

    ends = mlp(0, 2 * head)
    from_next = lax.ppermute(ends[head:], 'sp', down)
    from_prev = lax.ppermute(ends[:head], 'sp', up)
    middle = mlp(2 * head, n_cap - 2 * head)

    def give_back(cap):
        extra = max(cap - head, 0)

        def run():
            parts = [ends, middle, from_next, from_prev]
            stored = lax.rem(back_k + head, n_cap)
            place = jnp.where((back_k >= 0) & (back_k < n_cap), stored, 0)
            place = jnp.where((back_k >= n_cap) & (back_k < n_cap + head), back_k, place)
            place = jnp.where((back_k < 0) & (back_k >= -head), n_cap + 2 * head + back_k, place)
            size = n_cap + 2 * head
            if extra:
                over = max(cap + head - n_cap, 0)
                n_mid = extra - over
                parts.append(lax.ppermute(jnp.concatenate([middle[:n_mid], ends[:over]], axis=0), 'sp', down))
                parts.append(lax.ppermute(jnp.concatenate([ends[2 * head - over:], middle[middle.shape[0] - n_mid:]], axis=0), 'sp', up))
                place = jnp.where((back_k >= n_cap + head) & (back_k < n_cap + cap), size + back_k - n_cap - head, place)
                place = jnp.where((back_k < -head) & (back_k >= -cap), size + 2 * extra + head + back_k, place)
                size += 2 * extra
            parts.append(jnp.zeros((16, model_dim), hidden.dtype))
            place = jnp.where((back_k < -cap) | (back_k >= n_cap + cap), size, place)
            return jnp.concatenate(parts, axis=0).at[place].get(mode='promise_in_bounds')
        return run

    return lax.switch(bucket, [give_back(cap) for cap in levels])


def solution(mesh):
    row_spec = P(('dp', 'sp'), None)
    vec_spec = P(('dp', 'sp'))
    rep_spec = P()

    def per_device(hidden, tok_perm, send_off, send_len, recv_off, recv_len, recv_doc, recv_pos, *params):
        n_tok = hidden.shape[0]
        n_cap = recv_doc.shape[0]
        n_dev = send_off.shape[0]
        at_start = jnp.arange(n_cap, dtype=jnp.int32)[None, :] == recv_off[:, None]
        start_pos = jnp.sum(jnp.where(at_start, recv_pos[None, :], 0), axis=1)
        broken = jnp.sum(jnp.where(recv_len > 0, start_pos, 0))
        mine = jnp.concatenate([recv_pos, send_len, recv_off, jnp.full((112,), broken, jnp.int32)])
        every = lax.all_gather(mine, 'sp', axis=0)
        pos_all = every[:, :n_cap]
        send_all = every[:, n_cap:n_cap + n_dev]
        roff_all = every[:, n_cap + n_dev:n_cap + 2 * n_dev]
        totals, starts, offs = ring_plan(send_all, n_cap)
        prev_totals = jnp.concatenate([totals[-1:], totals[:-1]])
        fits = jnp.all((offs >= -prev_totals) & (offs <= totals) & (jnp.abs(offs) <= n_cap))
        whole = jnp.sum(jnp.abs(every[:, n_cap + 2 * n_dev])) == 0
        use_ring = fits & whole

        me = lax.axis_index('sp').astype(jnp.int32)
        ring_at = jnp.where(me < 4, me, me ^ 2)
        after = lax.rem(ring_at + 1, n_dev)
        off = jnp.clip(offs[ring_at], -n_cap, n_cap)
        off_next = jnp.clip(offs[after], -n_cap, n_cap)
        total = totals[ring_at]
        ext_idx = lax.dynamic_slice(jnp.pad(tok_perm, (2 * n_cap, 2 * n_cap)), (n_cap + off,), (3 * n_cap,))
        n_left = jnp.maximum(-off, 0)
        n_right = jnp.maximum(off_next, 0)
        reach = jnp.max(jnp.abs(offs))
        bucket = sum((reach > level).astype(jnp.int32) for level in LEVELS[:-1])

        order_of = ring_order(n_dev)
        runs = jnp.stack([send_all[d] for d in order_of])
        run_slot = jnp.stack([roff_all[:, d] for d in order_of])
        run_rel = starts[:, None] + jnp.cumsum(runs, axis=1) - runs - starts[ring_at] - off
        half = n_dev * n_cap // 2
        run_rel = jnp.where(run_rel >= half, run_rel - 2 * half, jnp.where(run_rel < -half, run_rel + 2 * half, run_rel))
        in_run = jnp.arange(n_cap, dtype=jnp.int32)[:, None] - run_rel.reshape(1, -1)
        run_base = (jnp.arange(n_dev, dtype=jnp.int32)[None, :] * every.shape[1] + run_slot).reshape(1, -1)
        from_at = jnp.sum(jnp.where((in_run >= 0) & (in_run < runs.reshape(1, -1)), run_base + in_run, 0), axis=1)
        plan = (ext_idx, from_at, every, off, total, n_left, n_right, bucket)

        def ring(_):
            return balanced_path(plan, hidden, tok_perm, *params)

        def general(_):
            return general_path(hidden, tok_perm, send_off, send_len, recv_off, recv_len, recv_doc, recv_pos, *params)

        return lax.cond(use_ring, ring, general, 0)

    return jax.shard_map(per_device, mesh=mesh, in_specs=(row_spec,) + (vec_spec,) * 7 + (rep_spec,) * 9, out_specs=row_spec, check_vma=False)
```

```python
import functools

import jax
import jax.numpy as jnp
from jax import lax
from jax.experimental import pallas as pl
from jax.experimental.layout import Layout, with_layout_constraint
from jax.experimental.pallas import tpu as pltpu
from jax.sharding import PartitionSpec as P

Q_BLOCK = 128
ROPE_BASE = 500000.0
NORM_EPS = 1e-5
NEG = -1e30
LOG2E = 1.4426950408889634

BQ = 512
BK = 512
HEAD_ROWS = 1024
ROW_TILE = 512
ZERO_ROWS = 1024
LEVELS = (1024, 1536, 2048, 3072)


def row_major(x):
    return with_layout_constraint(x, Layout(major_to_minor=tuple(range(x.ndim))))


def rms_norm(rows_in, gain_vec):
    rows_f = rows_in.astype(jnp.float32)
    inv_rms = lax.rsqrt(jnp.mean(rows_f * rows_f, axis=-1, keepdims=True) + NORM_EPS)
    return (rows_f * inv_rms * gain_vec.astype(jnp.float32)).astype(jnp.bfloat16)


def rope_tables(positions, head_dim):
    half_dim = head_dim // 2
    inv_freq = jnp.power(jnp.float32(ROPE_BASE), -2.0 * jnp.arange(half_dim, dtype=jnp.float32) / head_dim)
    angles = positions.astype(jnp.float32)[:, None] * inv_freq[None, :]
    return jnp.cos(angles), jnp.sin(angles)


def rope(proj, tables):
    cos_t, sin_t = tables[0][:, None, :], tables[1][:, None, :]
    half_dim = proj.shape[-1] // 2
    lo_half = proj[..., :half_dim]
    hi_half = proj[..., half_dim:]
    return jnp.concatenate([lo_half * cos_t - hi_half * sin_t, hi_half * cos_t + lo_half * sin_t], axis=-1)


def attend_general(q_rot, k_rot, v_proj, doc_ids, positions):
    n_rows, n_kv, q_per_kv, head_dim = q_rot.shape
    n_blocks = n_rows // Q_BLOCK
    qk_scale = head_dim ** -0.5

    def one_block(blk_args):
        q_blk, doc_q, pos_q = blk_args
        scores = jnp.einsum('qkgd,skd->kgqs', q_blk, k_rot, preferred_element_type=jnp.float32) * qk_scale
        allowed = (doc_q[:, None] == doc_ids[None, :]) & (positions[None, :] <= pos_q[:, None])
        probs_bf = jax.nn.softmax(jnp.where(allowed, scores, NEG), axis=-1).astype(jnp.bfloat16)
        return jnp.einsum('kgqs,skd->qkgd', probs_bf, v_proj, preferred_element_type=jnp.float32).astype(jnp.bfloat16)

    blocks_out = lax.map(one_block, (q_rot.reshape(n_blocks, Q_BLOCK, n_kv, q_per_kv, head_dim), doc_ids.reshape(n_blocks, Q_BLOCK), positions.reshape(n_blocks, Q_BLOCK)))
    return blocks_out.reshape(n_rows, n_kv * q_per_kv * head_dim)


def qkv(rows, positions, g_attn, w_q, w_k, w_v):
    normed = rms_norm(rows, g_attn)
    tables = lax.optimization_barrier(rope_tables(positions, w_q.shape[2]))
    k_proj = jnp.einsum('td,dhe->the', normed, w_k, preferred_element_type=jnp.float32)
    v_proj = jnp.einsum('td,dhe->the', normed, w_v, preferred_element_type=jnp.float32).astype(jnp.bfloat16)
    q_proj = jnp.einsum('td,dhe->the', normed, w_q, preferred_element_type=jnp.float32)
    return rope(q_proj, tables).astype(jnp.bfloat16), rope(k_proj, tables).astype(jnp.bfloat16), v_proj


def attn_residual(rows, attn_heads, w_o):
    attn_out = jnp.dot(attn_heads, w_o.reshape(-1, rows.shape[1]), preferred_element_type=jnp.float32).astype(jnp.bfloat16)
    return (rows.astype(jnp.float32) + attn_out.astype(jnp.float32)).astype(jnp.bfloat16)


def mlp_residual(resid_mid, g_mlp, w_gate, w_up, w_down):
    normed_mlp = rms_norm(resid_mid, g_mlp)
    gate_proj = jnp.dot(normed_mlp, w_gate, preferred_element_type=jnp.float32)
    up_proj = jnp.dot(normed_mlp, w_up, preferred_element_type=jnp.float32)
    hidden_act = (jax.nn.silu(gate_proj) * up_proj).astype(jnp.bfloat16)
    down_proj = jnp.dot(hidden_act, w_down, preferred_element_type=jnp.float32).astype(jnp.bfloat16)
    return (resid_mid.astype(jnp.float32) + down_proj.astype(jnp.float32)).astype(jnp.bfloat16)


def general_path(hidden, tok_perm, send_off, send_len, recv_off, recv_len, recv_doc, recv_pos, g_attn, w_q, w_k, w_v, w_o, g_mlp, w_gate, w_up, w_down):
    n_tok, model_dim = hidden.shape
    n_cap = recv_doc.shape[0]
    group_devs = send_off.shape[0]
    zero_val = jnp.zeros((), hidden.dtype)
    pair_row = jnp.arange(n_cap)[None, :]
    dev_base = jnp.arange(group_devs)[None, :] * n_cap
    send_idx = jnp.minimum(send_off[:, None] + pair_row, n_tok - 1).reshape(-1)
    send_buf = jnp.take(hidden, jnp.take(tok_perm, send_idx), axis=0).reshape(group_devs, n_cap, model_dim)
    recv_buf = lax.all_to_all(send_buf, 'sp', 0, 0, tiled=True).reshape(group_devs * n_cap, model_dim)
    slot_idx = jnp.arange(n_cap)[:, None]
    in_run = (slot_idx >= recv_off[None, :]) & (slot_idx < (recv_off + recv_len)[None, :])
    flat_pos = jnp.sum(jnp.where(in_run, dev_base + slot_idx - recv_off[None, :], 0), axis=1)
    rows = jnp.take(recv_buf, flat_pos, axis=0)
    q_rot, k_rot, v_proj = qkv(rows, recv_pos, g_attn, w_q, w_k, w_v)
    n_kv = w_k.shape[1]
    heads = attend_general(q_rot.reshape(n_cap, n_kv, -1, w_q.shape[2]), k_rot, v_proj, recv_doc, recv_pos)
    layer_rows = mlp_residual(attn_residual(rows, heads, w_o), g_mlp, w_gate, w_up, w_down)
    back_idx = jnp.minimum(recv_off[:, None] + pair_row, n_cap - 1).reshape(-1)
    back_buf = jnp.take(layer_rows, back_idx, axis=0).reshape(group_devs, n_cap, model_dim)
    back_recv = lax.all_to_all(back_buf, 'sp', 0, 0, tiled=True).reshape(group_devs * n_cap, model_dim)
    inv_perm = jnp.argsort(tok_perm)[:, None]
    in_back = (inv_perm >= send_off[None, :]) & (inv_perm < (send_off + send_len)[None, :])
    back_pos = jnp.sum(jnp.where(in_back, dev_base + inv_perm - send_off[None, :], 0), axis=1)
    was_sent = jnp.any(in_back, axis=1)
    return jnp.where(was_sent[:, None], jnp.take(back_recv, back_pos, axis=0), zero_val)


def flash_kernel(lomin_ref, lomax_ref, lo_ref, q_ref, k_ref, v_ref, o_ref, m_ref, l_ref, acc_ref, bias_ref, *, base, shift, scale):
    qb = pl.program_id(1)
    n_heads = q_ref.shape[1] // 128
    per_part = base // BK
    q_first = base + qb * BQ
    m_ref[...] = jnp.full(m_ref.shape, NEG, jnp.float32)
    l_ref[...] = jnp.zeros(l_ref.shape, jnp.float32)
    acc_ref[...] = jnp.zeros(acc_ref.shape, jnp.float32)

    def process(kb, masked):
        k_first = kb * BK
        part = kb // per_part
        stored = part * per_part + lax.rem(kb - part * per_part + shift // BK, per_part)
        k_rows = pl.ds(pl.multiple_of(stored * BK, BK), BK)
        k_blk = k_ref[k_rows, :]
        v_blk = v_ref[k_rows, :]
        if masked:
            k_idx = k_first + lax.broadcasted_iota(jnp.int32, (BQ, BK), 1)
            q_idx = q_first + lax.broadcasted_iota(jnp.int32, (BQ, BK), 0)
            ok = (k_idx >= lo_ref[...]) & (k_idx <= q_idx)
            bias_ref[...] = jnp.where(ok, 0.0, NEG)

        def score(n):
            return lax.dot_general(q_ref[:, n * 128:(n + 1) * 128], k_blk, (((1,), (1,)), ((), ())), preferred_element_type=jnp.float32)

        s_next = score(0)
        for n in range(n_heads):
            s = s_next
            if n + 1 < n_heads:
                s_next = score(n + 1)
            if masked:
                s = s + bias_ref[...]
            m_old = m_ref[n]
            m_new = jnp.maximum(m_old, jnp.max(s, axis=1, keepdims=True))
            alpha = jnp.exp2((m_old - m_new) * scale)
            p = jnp.exp2((s - jnp.concatenate([m_new] * (BK // 128), axis=1)) * scale)
            p_sum = p[:, :128]
            for c in range(128, BK, 128):
                p_sum = p_sum + p[:, c:c + 128]
            l_ref[n] = l_ref[n] * alpha + p_sum
            m_ref[n] = m_new
            pv = jnp.dot(p.astype(jnp.bfloat16), v_blk, preferred_element_type=jnp.float32)
            acc_ref[n] = acc_ref[n] * alpha + pv

    first = lomin_ref[qb] // BK
    last = (q_first + BQ - 1) // BK
    full_from = lomax_ref[qb]

    def step(kb, carry):
        inside = (kb * BK >= full_from) & ((kb + 1) * BK - 1 <= q_first)

        @pl.when(inside)
        def _():
            process(kb, False)

        @pl.when(jnp.logical_not(inside))
        def _():
            process(kb, True)

        return carry

    lax.fori_loop(first, last + 1, step, 0)
    for n in range(n_heads):
        o_ref[:, n * 128:(n + 1) * 128] = (acc_ref[n] / jnp.sum(l_ref[n], axis=1, keepdims=True)).astype(jnp.bfloat16)


def flash(q, kv, lo, shift):
    n_rows, width = q.shape
    n_kv = kv.shape[1] // 256
    group = width // n_kv
    n_q = n_rows // BQ
    blocks = lo.reshape(n_q, BQ)
    n_h = group // 128

    def q_at(h, i, *_):
        return lax.rem(i + shift // BQ, n_q), h

    return pl.pallas_call(
        functools.partial(flash_kernel, base=n_rows, shift=shift, scale=(128 ** -0.5) * LOG2E),
        grid_spec=pltpu.PrefetchScalarGridSpec(
            num_scalar_prefetch=2,
            grid=(n_kv, n_q),
            in_specs=[
                pl.BlockSpec((BQ, 1), lambda h, i, *_: (i, 0)),
                pl.BlockSpec((BQ, group), q_at),
                pl.BlockSpec((2 * n_rows, 128), lambda h, i, *_: (0, h)),
                pl.BlockSpec((2 * n_rows, 128), lambda h, i, *_: (0, n_kv + h)),
            ],
            out_specs=pl.BlockSpec((BQ, group), q_at),
            scratch_shapes=[
                pltpu.VMEM((n_h, BQ, 128), jnp.float32),
                pltpu.VMEM((n_h, BQ, 128), jnp.float32),
                pltpu.VMEM((n_h, BQ, 128), jnp.float32),
                pltpu.VMEM((BQ, BK), jnp.float32),
            ],
        ),
        out_shape=jax.ShapeDtypeStruct((n_rows, width), jnp.bfloat16),
        compiler_params=pltpu.CompilerParams(dimension_semantics=("arbitrary", "arbitrary")),
        cost_estimate=pl.CostEstimate(flops=80_000_000_000, bytes_accessed=40_000_000, transcendentals=80_000_000),
        name="flash",
    )(jnp.min(blocks, axis=1), jnp.max(blocks, axis=1), lo[:, None], q, kv, kv)


def norm_block(x_ref, g_ref, rows):
    x = x_ref[rows, :].astype(jnp.float32)
    inv = lax.rsqrt(jnp.mean(x * x, axis=1, keepdims=True) + NORM_EPS)
    return (x * inv * g_ref[...].astype(jnp.float32)).astype(jnp.bfloat16)


def proj_kernel(x_ref, g_ref, cos_ref, sin_ref, w_ref, o_ref, *, turned):
    h = norm_block(x_ref, g_ref, slice(None))
    width = w_ref.shape[1]
    for c in range(0, width, 256):
        y = jnp.dot(h, w_ref[:, c:c + 256], preferred_element_type=jnp.float32)
        for e in range(0, 256, 128):
            part = y[:, e:e + 128]
            if c + e < turned:
                part = part * cos_ref[...] + pltpu.roll(part, 64, 1) * sin_ref[...]
            o_ref[:, c + e:c + e + 128] = part.astype(jnp.bfloat16)


def project(x, gain, cos2, sin2, w, turned):
    n_rows, dim = x.shape
    width = w.shape[1]
    return pl.pallas_call(
        functools.partial(proj_kernel, turned=turned),
        grid=(n_rows // ROW_TILE,),
        in_specs=[
            pl.BlockSpec((ROW_TILE, dim), lambda i: (i, 0)),
            pl.BlockSpec((1, dim), lambda i: (0, 0)),
            pl.BlockSpec((ROW_TILE, 128), lambda i: (i, 0)),
            pl.BlockSpec((ROW_TILE, 128), lambda i: (i, 0)),
            pl.BlockSpec((dim, width), lambda i: (0, 0)),
        ],
        out_specs=pl.BlockSpec((ROW_TILE, width), lambda i: (i, 0)),
        out_shape=jax.ShapeDtypeStruct((n_rows, width), jnp.bfloat16),
        compiler_params=pltpu.CompilerParams(dimension_semantics=("arbitrary",)),
        cost_estimate=pl.CostEstimate(flops=2 * n_rows * dim * width, bytes_accessed=2 * (n_rows * (dim + width) + dim * width), transcendentals=0),
        name="project",
    )(x, gain[None, :], cos2, sin2, w)


def gate_up_kernel(z_ref, g_ref, wg_ref, wu_ref, o_ref, h_ref):
    n_rows = z_ref.shape[0]

    @pl.when(pl.program_id(0) == 0)
    def _():
        for r in range(0, n_rows, 256):
            h_ref[r:r + 256, :] = norm_block(z_ref, g_ref, slice(r, r + 256))

    for r in range(0, n_rows, ROW_TILE):
        h = h_ref[r:r + ROW_TILE, :]
        gate = jnp.dot(h, wg_ref[...], preferred_element_type=jnp.float32)
        up = jnp.dot(h, wu_ref[...], preferred_element_type=jnp.float32)
        o_ref[r:r + ROW_TILE, :] = (jax.nn.silu(gate) * up).astype(jnp.bfloat16)


def gate_up(z, first, n_rows, gain, w_gate, w_up, tile=256):
    dim = z.shape[1]
    ff = w_gate.shape[1]
    return pl.pallas_call(
        gate_up_kernel,
        grid=(ff // tile,),
        in_specs=[
            pl.BlockSpec((n_rows, dim), lambda j: (first // n_rows, 0)),
            pl.BlockSpec((1, dim), lambda j: (0, 0)),
            pl.BlockSpec((dim, tile), lambda j: (0, j)),
            pl.BlockSpec((dim, tile), lambda j: (0, j)),
        ],
        out_specs=pl.BlockSpec((n_rows, tile), lambda j: (0, j)),
        out_shape=jax.ShapeDtypeStruct((n_rows, ff), jnp.bfloat16),
        scratch_shapes=[pltpu.VMEM((n_rows, dim), jnp.bfloat16)],
        compiler_params=pltpu.CompilerParams(dimension_semantics=("arbitrary",)),
        cost_estimate=pl.CostEstimate(flops=4 * n_rows * dim * ff, bytes_accessed=2 * (n_rows * (dim + ff) + 2 * dim * ff), transcendentals=n_rows * ff),
        name="gate_up",
    )(z, gain[None, :], w_gate, w_up)


def ring_perm(n_dev, shift):
    order = ring_order(n_dev)
    return [(order[r], order[(r + shift) % n_dev]) for r in range(n_dev)]


def ring_order(n_dev):
    return [0, 1, 2, 3, 6, 7, 4, 5]


def ring_plan(send_len_all, n_cap):
    n_dev = send_len_all.shape[0]
    totals = jnp.sum(send_len_all, axis=1)
    totals = jnp.stack([totals[d] for d in ring_order(n_dev)])
    ends = jnp.cumsum(totals)
    excess = ends - totals - n_cap * jnp.arange(n_dev, dtype=jnp.int32)
    centre = (jnp.max(excess) + jnp.min(excess)) // 2
    return totals, ends - totals, centre - excess


def balanced_path(plan, hidden, tok_perm, g_attn, w_q, w_k, w_v, w_o, g_mlp, w_gate, w_up, w_down):
    ext_idx, from_at, every, off, total, n_left, n_right, bucket = plan
    model_dim = hidden.shape[1]
    n_cap = from_at.shape[0]
    n_dev = 8
    head = HEAD_ROWS
    up, down = ring_perm(n_dev, 1), ring_perm(n_dev, -1)
    slot = jnp.arange(n_cap, dtype=jnp.int32)
    levels = LEVELS
    n_kv, head_dim = w_k.shape[1:]

    def grab(idx):
        return hidden.at[idx].get(mode='promise_in_bounds')

    def exchange(cap):
        def run():
            right = lax.ppermute(grab(ext_idx[n_cap - cap:n_cap]), 'sp', down)
            left = lax.ppermute(grab(ext_idx[2 * n_cap:2 * n_cap + cap]), 'sp', up)
            rows = row_major(grab(jnp.roll(ext_idx[n_cap:2 * n_cap], head)))
            pos = every.reshape(-1).at[from_at].get(mode='promise_in_bounds')
            cos_t, sin_t = rope_tables(jnp.roll(pos, head), head_dim)
            cos2 = jnp.concatenate([cos_t, cos_t], axis=1)
            sin2 = jnp.concatenate([-sin_t, sin_t], axis=1)
            order = jnp.argsort(tok_perm)
            back_k = jnp.where(order < total, order - off, 4 * n_cap).astype(jnp.int32)
            w_kv = jnp.concatenate([w_k.reshape(model_dim, -1), w_v.reshape(model_dim, -1)], axis=1)

            def merge(rows, stored, vals, keep):
                size = vals.shape[0]
                return rows.at[stored:stored + size].set(jnp.where(keep[:, None], vals, rows[stored:stored + size]))

            step = jnp.arange(cap, dtype=jnp.int32)
            keep_l, keep_r = step < n_left, step >= cap - n_right
            cut = min(cap, n_cap - head)
            rows = merge(rows, head, left[:cut], keep_l[:cut])
            if cap > cut:
                rows = merge(rows, 0, left[cut:], keep_l[cut:])
            cut = max(cap - head, 0)
            rows = merge(rows, 0, right[cut:], keep_r[cut:])
            if cut:
                rows = merge(rows, n_cap - cut, right[:cut], keep_r[:cut])
            return rows, pos, cos2, sin2, back_k, w_q.reshape(model_dim, -1), w_kv
        return run

    rows, pos, cos2, sin2, back_k, w_q2, w_kv = lax.switch(bucket, [exchange(cap) for cap in levels])
    rows = row_major(rows)
    kv = project(rows, g_attn, cos2, sin2, w_kv, n_kv * head_dim)
    kv_prev = lax.ppermute(kv, 'sp', up)
    q_rot = project(rows, g_attn, cos2, sin2, w_q2, w_q2.shape[1])
    kv = jnp.concatenate([kv_prev, kv], axis=0)
    heads = flash(q_rot, kv, n_cap + slot - pos, head)
    resid_mid = row_major(attn_residual(rows, heads, w_o))

    def mlp(first, n_rows):
        z = resid_mid[first:first + n_rows]
        acts = gate_up(resid_mid, first, n_rows, g_mlp, w_gate, w_up)
        down_proj = jnp.dot(acts, w_down, preferred_element_type=jnp.float32).astype(jnp.bfloat16)
        return row_major((z.astype(jnp.float32) + down_proj.astype(jnp.float32)).astype(jnp.bfloat16))

    ends = mlp(0, 2 * head)
    from_next = lax.ppermute(ends[head:], 'sp', down)
    from_prev = lax.ppermute(ends[:head], 'sp', up)
    middle = mlp(2 * head, n_cap - 2 * head)

    def give_back(cap):
        extra = max(cap - head, 0)

        def run():
            parts = [ends, middle, from_next, from_prev]
            stored = lax.rem(back_k + head, n_cap)
            place = jnp.where((back_k >= 0) & (back_k < n_cap), stored, 0)
            place = jnp.where((back_k >= n_cap) & (back_k < n_cap + head), back_k, place)
            place = jnp.where((back_k < 0) & (back_k >= -head), n_cap + 2 * head + back_k, place)
            size = n_cap + 2 * head
            if extra:
                over = max(cap + head - n_cap, 0)
                n_mid = extra - over
                parts.append(lax.ppermute(jnp.concatenate([middle[:n_mid], ends[:over]], axis=0), 'sp', down))
                parts.append(lax.ppermute(jnp.concatenate([ends[2 * head - over:], middle[middle.shape[0] - n_mid:]], axis=0), 'sp', up))
                place = jnp.where((back_k >= n_cap + head) & (back_k < n_cap + cap), size + back_k - n_cap - head, place)
                place = jnp.where((back_k < -head) & (back_k >= -cap), size + 2 * extra + head + back_k, place)
                size += 2 * extra
            parts.append(jnp.zeros((ZERO_ROWS, model_dim), hidden.dtype))
            zero_at = size + lax.rem(jnp.arange(back_k.shape[0], dtype=jnp.int32), ZERO_ROWS)
            place = jnp.where((back_k < -cap) | (back_k >= n_cap + cap), zero_at, place)
            return jnp.concatenate(parts, axis=0).at[place].get(mode='promise_in_bounds')
        return run

    return lax.switch(bucket, [give_back(cap) for cap in levels])


def solution(mesh):
    row_spec = P(('dp', 'sp'), None)
    vec_spec = P(('dp', 'sp'))
    rep_spec = P()

    def per_device(hidden, tok_perm, send_off, send_len, recv_off, recv_len, recv_doc, recv_pos, *params):
        n_tok = hidden.shape[0]
        n_cap = recv_doc.shape[0]
        n_dev = send_off.shape[0]
        at_start = jnp.arange(n_cap, dtype=jnp.int32)[None, :] == recv_off[:, None]
        start_pos = jnp.sum(jnp.where(at_start, recv_pos[None, :], 0), axis=1)
        broken = jnp.sum(jnp.where(recv_len > 0, start_pos, 0))
        mine = jnp.concatenate([recv_pos, send_len, recv_off, jnp.full((112,), broken, jnp.int32)])
        every = lax.all_gather(mine, 'sp', axis=0)
        pos_all = every[:, :n_cap]
        send_all = every[:, n_cap:n_cap + n_dev]
        roff_all = every[:, n_cap + n_dev:n_cap + 2 * n_dev]
        totals, starts, offs = ring_plan(send_all, n_cap)
        prev_totals = jnp.concatenate([totals[-1:], totals[:-1]])
        fits = jnp.all((offs >= -prev_totals) & (offs <= totals) & (jnp.abs(offs) <= n_cap))
        whole = jnp.sum(jnp.abs(every[:, n_cap + 2 * n_dev])) == 0
        use_ring = fits & whole

        me = lax.axis_index('sp').astype(jnp.int32)
        ring_at = jnp.where(me < 4, me, me ^ 2)
        after = lax.rem(ring_at + 1, n_dev)
        off = jnp.clip(offs[ring_at], -n_cap, n_cap)
        off_next = jnp.clip(offs[after], -n_cap, n_cap)
        total = totals[ring_at]
        spread = jnp.arange(2 * n_cap, dtype=jnp.int32)
        ext_idx = lax.dynamic_slice(jnp.concatenate([spread, tok_perm, spread]), (n_cap + off,), (3 * n_cap,))
        n_left = jnp.maximum(-off, 0)
        n_right = jnp.maximum(off_next, 0)
        reach = jnp.max(jnp.abs(offs))
        bucket = sum((reach > level).astype(jnp.int32) for level in LEVELS[:-1])

        order_of = ring_order(n_dev)
        runs = jnp.stack([send_all[d] for d in order_of])
        run_slot = jnp.stack([roff_all[:, d] for d in order_of])
        run_rel = starts[:, None] + jnp.cumsum(runs, axis=1) - runs - starts[ring_at] - off
        half = n_dev * n_cap // 2
        run_rel = jnp.where(run_rel >= half, run_rel - 2 * half, jnp.where(run_rel < -half, run_rel + 2 * half, run_rel))
        in_run = jnp.arange(n_cap, dtype=jnp.int32)[:, None] - run_rel.reshape(1, -1)
        run_base = (jnp.arange(n_dev, dtype=jnp.int32)[None, :] * every.shape[1] + run_slot).reshape(1, -1)
        from_at = jnp.sum(jnp.where((in_run >= 0) & (in_run < runs.reshape(1, -1)), run_base + in_run, 0), axis=1)
        plan = (ext_idx, from_at, every, off, total, n_left, n_right, bucket)

        def ring(_):
            return balanced_path(plan, hidden, tok_perm, *params)

        def general(_):
            return general_path(hidden, tok_perm, send_off, send_len, recv_off, recv_len, recv_doc, recv_pos, *params)

        return lax.cond(use_ring, ring, general, 0)

    return jax.shard_map(per_device, mesh=mesh, in_specs=(row_spec,) + (vec_spec,) * 7 + (rep_spec,) * 9, out_specs=row_spec, check_vma=False)
```

```python
import functools

import jax
import jax.numpy as jnp
from jax import lax
from jax.experimental import pallas as pl
from jax.experimental.layout import Layout, with_layout_constraint
from jax.experimental.pallas import tpu as pltpu
from jax.sharding import PartitionSpec as P

Q_BLOCK = 128
ROPE_BASE = 500000.0
NORM_EPS = 1e-5
NEG = -1e30
LOG2E = 1.4426950408889634

BQ = 512
BK = 512
HEAD_ROWS = 1024
ROW_TILE = 512
ZERO_ROWS = 256
LEVELS = (1024, 1536, 2048, 3072)


def row_major(x):
    return with_layout_constraint(x, Layout(major_to_minor=tuple(range(x.ndim))))


def rms_norm(rows_in, gain_vec):
    rows_f = rows_in.astype(jnp.float32)
    inv_rms = lax.rsqrt(jnp.mean(rows_f * rows_f, axis=-1, keepdims=True) + NORM_EPS)
    return (rows_f * inv_rms * gain_vec.astype(jnp.float32)).astype(jnp.bfloat16)


def rope_tables(positions, head_dim):
    half_dim = head_dim // 2
    inv_freq = jnp.power(jnp.float32(ROPE_BASE), -2.0 * jnp.arange(half_dim, dtype=jnp.float32) / head_dim)
    angles = positions.astype(jnp.float32)[:, None] * inv_freq[None, :]
    return jnp.cos(angles), jnp.sin(angles)


def rope(proj, tables):
    cos_t, sin_t = tables[0][:, None, :], tables[1][:, None, :]
    half_dim = proj.shape[-1] // 2
    lo_half = proj[..., :half_dim]
    hi_half = proj[..., half_dim:]
    return jnp.concatenate([lo_half * cos_t - hi_half * sin_t, hi_half * cos_t + lo_half * sin_t], axis=-1)


def attend_general(q_rot, k_rot, v_proj, doc_ids, positions):
    n_rows, n_kv, q_per_kv, head_dim = q_rot.shape
    n_blocks = n_rows // Q_BLOCK
    qk_scale = head_dim ** -0.5

    def one_block(blk_args):
        q_blk, doc_q, pos_q = blk_args
        scores = jnp.einsum('qkgd,skd->kgqs', q_blk, k_rot, preferred_element_type=jnp.float32) * qk_scale
        allowed = (doc_q[:, None] == doc_ids[None, :]) & (positions[None, :] <= pos_q[:, None])
        probs_bf = jax.nn.softmax(jnp.where(allowed, scores, NEG), axis=-1).astype(jnp.bfloat16)
        return jnp.einsum('kgqs,skd->qkgd', probs_bf, v_proj, preferred_element_type=jnp.float32).astype(jnp.bfloat16)

    blocks_out = lax.map(one_block, (q_rot.reshape(n_blocks, Q_BLOCK, n_kv, q_per_kv, head_dim), doc_ids.reshape(n_blocks, Q_BLOCK), positions.reshape(n_blocks, Q_BLOCK)))
    return blocks_out.reshape(n_rows, n_kv * q_per_kv * head_dim)


def qkv(rows, positions, g_attn, w_q, w_k, w_v):
    normed = rms_norm(rows, g_attn)
    tables = lax.optimization_barrier(rope_tables(positions, w_q.shape[2]))
    k_proj = jnp.einsum('td,dhe->the', normed, w_k, preferred_element_type=jnp.float32)
    v_proj = jnp.einsum('td,dhe->the', normed, w_v, preferred_element_type=jnp.float32).astype(jnp.bfloat16)
    q_proj = jnp.einsum('td,dhe->the', normed, w_q, preferred_element_type=jnp.float32)
    return rope(q_proj, tables).astype(jnp.bfloat16), rope(k_proj, tables).astype(jnp.bfloat16), v_proj


def attn_residual(rows, attn_heads, w_o):
    attn_out = jnp.dot(attn_heads, w_o.reshape(-1, rows.shape[1]), preferred_element_type=jnp.float32).astype(jnp.bfloat16)
    return (rows.astype(jnp.float32) + attn_out.astype(jnp.float32)).astype(jnp.bfloat16)


def mlp_residual(resid_mid, g_mlp, w_gate, w_up, w_down):
    normed_mlp = rms_norm(resid_mid, g_mlp)
    gate_proj = jnp.dot(normed_mlp, w_gate, preferred_element_type=jnp.float32)
    up_proj = jnp.dot(normed_mlp, w_up, preferred_element_type=jnp.float32)
    hidden_act = (jax.nn.silu(gate_proj) * up_proj).astype(jnp.bfloat16)
    down_proj = jnp.dot(hidden_act, w_down, preferred_element_type=jnp.float32).astype(jnp.bfloat16)
    return (resid_mid.astype(jnp.float32) + down_proj.astype(jnp.float32)).astype(jnp.bfloat16)


def general_path(hidden, tok_perm, send_off, send_len, recv_off, recv_len, recv_doc, recv_pos, g_attn, w_q, w_k, w_v, w_o, g_mlp, w_gate, w_up, w_down):
    n_tok, model_dim = hidden.shape
    n_cap = recv_doc.shape[0]
    group_devs = send_off.shape[0]
    zero_val = jnp.zeros((), hidden.dtype)
    pair_row = jnp.arange(n_cap)[None, :]
    dev_base = jnp.arange(group_devs)[None, :] * n_cap
    send_idx = jnp.minimum(send_off[:, None] + pair_row, n_tok - 1).reshape(-1)
    send_buf = jnp.take(hidden, jnp.take(tok_perm, send_idx), axis=0).reshape(group_devs, n_cap, model_dim)
    recv_buf = lax.all_to_all(send_buf, 'sp', 0, 0, tiled=True).reshape(group_devs * n_cap, model_dim)
    slot_idx = jnp.arange(n_cap)[:, None]
    in_run = (slot_idx >= recv_off[None, :]) & (slot_idx < (recv_off + recv_len)[None, :])
    flat_pos = jnp.sum(jnp.where(in_run, dev_base + slot_idx - recv_off[None, :], 0), axis=1)
    rows = jnp.take(recv_buf, flat_pos, axis=0)
    q_rot, k_rot, v_proj = qkv(rows, recv_pos, g_attn, w_q, w_k, w_v)
    n_kv = w_k.shape[1]
    heads = attend_general(q_rot.reshape(n_cap, n_kv, -1, w_q.shape[2]), k_rot, v_proj, recv_doc, recv_pos)
    layer_rows = mlp_residual(attn_residual(rows, heads, w_o), g_mlp, w_gate, w_up, w_down)
    back_idx = jnp.minimum(recv_off[:, None] + pair_row, n_cap - 1).reshape(-1)
    back_buf = jnp.take(layer_rows, back_idx, axis=0).reshape(group_devs, n_cap, model_dim)
    back_recv = lax.all_to_all(back_buf, 'sp', 0, 0, tiled=True).reshape(group_devs * n_cap, model_dim)
    inv_perm = jnp.argsort(tok_perm)[:, None]
    in_back = (inv_perm >= send_off[None, :]) & (inv_perm < (send_off + send_len)[None, :])
    back_pos = jnp.sum(jnp.where(in_back, dev_base + inv_perm - send_off[None, :], 0), axis=1)
    was_sent = jnp.any(in_back, axis=1)
    return jnp.where(was_sent[:, None], jnp.take(back_recv, back_pos, axis=0), zero_val)


def flash_kernel(lomin_ref, lomax_ref, lo_ref, q_ref, k_ref, v_ref, o_ref, m_ref, l_ref, acc_ref, bias_ref, *, base, shift, scale):
    qb = pl.program_id(1)
    n_heads = q_ref.shape[1] // 128
    per_part = base // BK
    q_first = base + qb * BQ
    m_ref[...] = jnp.full(m_ref.shape, NEG, jnp.float32)
    l_ref[...] = jnp.zeros(l_ref.shape, jnp.float32)
    acc_ref[...] = jnp.zeros(acc_ref.shape, jnp.float32)

    def process(kb, masked):
        k_first = kb * BK
        part = kb // per_part
        stored = part * per_part + lax.rem(kb - part * per_part + shift // BK, per_part)
        k_rows = pl.ds(pl.multiple_of(stored * BK, BK), BK)
        k_blk = k_ref[k_rows, :]
        v_blk = v_ref[k_rows, :]
        if masked:
            k_idx = k_first + lax.broadcasted_iota(jnp.int32, (BQ, BK), 1)
            q_idx = q_first + lax.broadcasted_iota(jnp.int32, (BQ, BK), 0)
            ok = (k_idx >= lo_ref[...]) & (k_idx <= q_idx)
            bias_ref[...] = jnp.where(ok, 0.0, NEG)

        def score(n):
            return lax.dot_general(q_ref[:, n * 128:(n + 1) * 128], k_blk, (((1,), (1,)), ((), ())), preferred_element_type=jnp.float32)

        s_next = score(0)
        for n in range(n_heads):
            s = s_next
            if n + 1 < n_heads:
                s_next = score(n + 1)
            if masked:
                s = s + bias_ref[...]
            m_old = m_ref[n]
            m_new = jnp.maximum(m_old, jnp.max(s, axis=1, keepdims=True))
            alpha = jnp.exp2((m_old - m_new) * scale)
            p = jnp.exp2((s - jnp.concatenate([m_new] * (BK // 128), axis=1)) * scale)
            p_sum = p[:, :128]
            for c in range(128, BK, 128):
                p_sum = p_sum + p[:, c:c + 128]
            l_ref[n] = l_ref[n] * alpha + p_sum
            m_ref[n] = m_new
            pv = jnp.dot(p.astype(jnp.bfloat16), v_blk, preferred_element_type=jnp.float32)
            acc_ref[n] = acc_ref[n] * alpha + pv

    first = lomin_ref[qb] // BK
    last = (q_first + BQ - 1) // BK
    full_from = lomax_ref[qb]

    def step(kb, carry):
        inside = (kb * BK >= full_from) & ((kb + 1) * BK - 1 <= q_first)

        @pl.when(inside)
        def _():
            process(kb, False)

        @pl.when(jnp.logical_not(inside))
        def _():
            process(kb, True)

        return carry

    lax.fori_loop(first, last + 1, step, 0)
    for n in range(n_heads):
        o_ref[:, n * 128:(n + 1) * 128] = (acc_ref[n] / jnp.sum(l_ref[n], axis=1, keepdims=True)).astype(jnp.bfloat16)


def flash(q, kv, lo, shift):
    n_rows, width = q.shape
    n_kv = kv.shape[1] // 256
    group = width // n_kv
    n_q = n_rows // BQ
    blocks = lo.reshape(n_q, BQ)
    n_h = group // 128

    def q_at(h, i, *_):
        return lax.rem(i + shift // BQ, n_q), h

    return pl.pallas_call(
        functools.partial(flash_kernel, base=n_rows, shift=shift, scale=(128 ** -0.5) * LOG2E),
        grid_spec=pltpu.PrefetchScalarGridSpec(
            num_scalar_prefetch=2,
            grid=(n_kv, n_q),
            in_specs=[
                pl.BlockSpec((BQ, 1), lambda h, i, *_: (i, 0)),
                pl.BlockSpec((BQ, group), q_at),
                pl.BlockSpec((2 * n_rows, 128), lambda h, i, *_: (0, h)),
                pl.BlockSpec((2 * n_rows, 128), lambda h, i, *_: (0, n_kv + h)),
            ],
            out_specs=pl.BlockSpec((BQ, group), q_at),
            scratch_shapes=[
                pltpu.VMEM((n_h, BQ, 128), jnp.float32),
                pltpu.VMEM((n_h, BQ, 128), jnp.float32),
                pltpu.VMEM((n_h, BQ, 128), jnp.float32),
                pltpu.VMEM((BQ, BK), jnp.float32),
            ],
        ),
        out_shape=jax.ShapeDtypeStruct((n_rows, width), jnp.bfloat16),
        compiler_params=pltpu.CompilerParams(dimension_semantics=("arbitrary", "arbitrary")),
        cost_estimate=pl.CostEstimate(flops=80_000_000_000, bytes_accessed=40_000_000, transcendentals=80_000_000),
        name="flash",
    )(jnp.min(blocks, axis=1), jnp.max(blocks, axis=1), lo[:, None], q, kv, kv)


def norm_block(x_ref, g_ref, rows):
    x = x_ref[rows, :].astype(jnp.float32)
    inv = lax.rsqrt(jnp.mean(x * x, axis=1, keepdims=True) + NORM_EPS)
    return (x * inv * g_ref[...].astype(jnp.float32)).astype(jnp.bfloat16)


def proj_kernel(x_ref, g_ref, cos_ref, sin_ref, w_ref, o_ref, *, turned):
    h = norm_block(x_ref, g_ref, slice(None))
    width = w_ref.shape[1]
    for c in range(0, width, 256):
        y = jnp.dot(h, w_ref[:, c:c + 256], preferred_element_type=jnp.float32)
        for e in range(0, 256, 128):
            part = y[:, e:e + 128]
            if c + e < turned:
                part = part * cos_ref[...] + pltpu.roll(part, 64, 1) * sin_ref[...]
            o_ref[:, c + e:c + e + 128] = part.astype(jnp.bfloat16)


def project(x, gain, cos2, sin2, w, turned):
    n_rows, dim = x.shape
    width = w.shape[1]
    return pl.pallas_call(
        functools.partial(proj_kernel, turned=turned),
        grid=(n_rows // ROW_TILE,),
        in_specs=[
            pl.BlockSpec((ROW_TILE, dim), lambda i: (i, 0)),
            pl.BlockSpec((1, dim), lambda i: (0, 0)),
            pl.BlockSpec((ROW_TILE, 128), lambda i: (i, 0)),
            pl.BlockSpec((ROW_TILE, 128), lambda i: (i, 0)),
            pl.BlockSpec((dim, width), lambda i: (0, 0)),
        ],
        out_specs=pl.BlockSpec((ROW_TILE, width), lambda i: (i, 0)),
        out_shape=jax.ShapeDtypeStruct((n_rows, width), jnp.bfloat16),
        compiler_params=pltpu.CompilerParams(dimension_semantics=("arbitrary",)),
        cost_estimate=pl.CostEstimate(flops=2 * n_rows * dim * width, bytes_accessed=2 * (n_rows * (dim + width) + dim * width), transcendentals=0),
        name="project",
    )(x, gain[None, :], cos2, sin2, w)


def gate_up_kernel(z_ref, g_ref, wg_ref, wu_ref, o_ref, h_ref):
    n_rows = z_ref.shape[0]

    @pl.when(pl.program_id(0) == 0)
    def _():
        for r in range(0, n_rows, 256):
            h_ref[r:r + 256, :] = norm_block(z_ref, g_ref, slice(r, r + 256))

    for r in range(0, n_rows, ROW_TILE):
        h = h_ref[r:r + ROW_TILE, :]
        gate = jnp.dot(h, wg_ref[...], preferred_element_type=jnp.float32)
        up = jnp.dot(h, wu_ref[...], preferred_element_type=jnp.float32)
        o_ref[r:r + ROW_TILE, :] = (jax.nn.silu(gate) * up).astype(jnp.bfloat16)


def gate_up(z, first, n_rows, gain, w_gate, w_up, tile=256):
    dim = z.shape[1]
    ff = w_gate.shape[1]
    return pl.pallas_call(
        gate_up_kernel,
        grid=(ff // tile,),
        in_specs=[
            pl.BlockSpec((n_rows, dim), lambda j: (first // n_rows, 0)),
            pl.BlockSpec((1, dim), lambda j: (0, 0)),
            pl.BlockSpec((dim, tile), lambda j: (0, j)),
            pl.BlockSpec((dim, tile), lambda j: (0, j)),
        ],
        out_specs=pl.BlockSpec((n_rows, tile), lambda j: (0, j)),
        out_shape=jax.ShapeDtypeStruct((n_rows, ff), jnp.bfloat16),
        scratch_shapes=[pltpu.VMEM((n_rows, dim), jnp.bfloat16)],
        compiler_params=pltpu.CompilerParams(dimension_semantics=("arbitrary",)),
        cost_estimate=pl.CostEstimate(flops=4 * n_rows * dim * ff, bytes_accessed=2 * (n_rows * (dim + ff) + 2 * dim * ff), transcendentals=n_rows * ff),
        name="gate_up",
    )(z, gain[None, :], w_gate, w_up)


def ring_perm(n_dev, shift):
    order = ring_order(n_dev)
    return [(order[r], order[(r + shift) % n_dev]) for r in range(n_dev)]


def ring_order(n_dev):
    return [0, 1, 2, 3, 6, 7, 4, 5]


def ring_plan(send_len_all, n_cap):
    n_dev = send_len_all.shape[0]
    totals = jnp.sum(send_len_all, axis=1)
    totals = jnp.stack([totals[d] for d in ring_order(n_dev)])
    ends = jnp.cumsum(totals)
    excess = ends - totals - n_cap * jnp.arange(n_dev, dtype=jnp.int32)
    centre = (jnp.max(excess) + jnp.min(excess)) // 2
    return totals, ends - totals, centre - excess


def balanced_path(plan, hidden, tok_perm, g_attn, w_q, w_k, w_v, w_o, g_mlp, w_gate, w_up, w_down):
    ext_idx, from_at, every, off, total, n_left, n_right, bucket = plan
    model_dim = hidden.shape[1]
    n_cap = from_at.shape[0]
    n_dev = 8
    head = HEAD_ROWS
    up, down = ring_perm(n_dev, 1), ring_perm(n_dev, -1)
    slot = jnp.arange(n_cap, dtype=jnp.int32)
    levels = LEVELS
    n_kv, head_dim = w_k.shape[1:]

    def grab(idx):
        return hidden.at[idx].get(mode='promise_in_bounds')

    def exchange(cap):
        def run():
            right = lax.ppermute(grab(ext_idx[n_cap - cap:n_cap]), 'sp', down)
            left = lax.ppermute(grab(ext_idx[2 * n_cap:2 * n_cap + cap]), 'sp', up)
            rows = row_major(grab(jnp.roll(ext_idx[n_cap:2 * n_cap], head)))
            pos = every.reshape(-1).at[from_at].get(mode='promise_in_bounds')
            cos_t, sin_t = rope_tables(jnp.roll(pos, head), head_dim)
            cos2 = jnp.concatenate([cos_t, cos_t], axis=1)
            sin2 = jnp.concatenate([-sin_t, sin_t], axis=1)
            order = jnp.argsort(tok_perm)
            back_k = jnp.where(order < total, order - off, 4 * n_cap).astype(jnp.int32)
            w_kv = jnp.concatenate([w_k.reshape(model_dim, -1), w_v.reshape(model_dim, -1)], axis=1)

            def merge(rows, stored, vals, keep):
                size = vals.shape[0]
                return rows.at[stored:stored + size].set(jnp.where(keep[:, None], vals, rows[stored:stored + size]))

            step = jnp.arange(cap, dtype=jnp.int32)
            keep_l, keep_r = step < n_left, step >= cap - n_right
            cut = min(cap, n_cap - head)
            rows = merge(rows, head, left[:cut], keep_l[:cut])
            if cap > cut:
                rows = merge(rows, 0, left[cut:], keep_l[cut:])
            cut = max(cap - head, 0)
            rows = merge(rows, 0, right[cut:], keep_r[cut:])
            if cut:
                rows = merge(rows, n_cap - cut, right[:cut], keep_r[:cut])
            return rows, pos, cos2, sin2, back_k, w_q.reshape(model_dim, -1), w_kv
        return run

    rows, pos, cos2, sin2, back_k, w_q2, w_kv = lax.switch(bucket, [exchange(cap) for cap in levels])
    rows = row_major(rows)
    kv = project(rows, g_attn, cos2, sin2, w_kv, n_kv * head_dim)
    kv_prev = lax.ppermute(kv, 'sp', up)
    q_rot = project(rows, g_attn, cos2, sin2, w_q2, w_q2.shape[1])
    kv = jnp.concatenate([kv_prev, kv], axis=0)
    heads = flash(q_rot, kv, n_cap + slot - pos, head)
    resid_mid = row_major(attn_residual(rows, heads, w_o))

    def mlp(first, n_rows):
        z = resid_mid[first:first + n_rows]
        acts = gate_up(resid_mid, first, n_rows, g_mlp, w_gate, w_up)
        down_proj = jnp.dot(acts, w_down, preferred_element_type=jnp.float32).astype(jnp.bfloat16)
        return row_major((z.astype(jnp.float32) + down_proj.astype(jnp.float32)).astype(jnp.bfloat16))

    ends = mlp(0, 2 * head)
    from_next = lax.ppermute(ends[head:], 'sp', down)
    from_prev = lax.ppermute(ends[:head], 'sp', up)
    middle = mlp(2 * head, n_cap - 2 * head)

    def give_back(cap):
        extra = max(cap - head, 0)

        def run():
            to_us, from_before = [from_next], [from_prev]
            if extra:
                over = max(cap + head - n_cap, 0)
                n_mid = extra - over
                to_us.append(lax.ppermute(jnp.concatenate([middle[:n_mid], ends[:over]], axis=0), 'sp', down))
                from_before.insert(0, lax.ppermute(jnp.concatenate([ends[2 * head - over:], middle[middle.shape[0] - n_mid:]], axis=0), 'sp', up))
            size = min(2 * cap, n_cap)
            both = 2 * cap - size
            nxt, prv = jnp.concatenate(to_us, axis=0), jnp.concatenate(from_before, axis=0)
            parts = [ends, middle, nxt[:cap - both]]
            if both:
                at = jnp.arange(cap - both, cap, dtype=jnp.int32)[:, None]
                parts.append(jnp.where(at < total - off - n_cap, nxt[cap - both:], prv[:both]))
            parts += [prv[both:], jnp.zeros((ZERO_ROWS, model_dim), hidden.dtype)]
            place = n_cap + size + lax.rem(jnp.arange(back_k.shape[0], dtype=jnp.int32), ZERO_ROWS)
            place = jnp.where((back_k >= 0) & (back_k < n_cap), lax.rem(back_k + head, n_cap), place)
            place = jnp.where((back_k >= n_cap) & (back_k < n_cap + cap), back_k, place)
            place = jnp.where((back_k < 0) & (back_k >= -cap), n_cap + size + back_k, place)
            return jnp.concatenate(parts, axis=0).at[place].get(mode='promise_in_bounds')
        return run

    return lax.switch(bucket, [give_back(cap) for cap in levels])


def solution(mesh):
    row_spec = P(('dp', 'sp'), None)
    vec_spec = P(('dp', 'sp'))
    rep_spec = P()

    def per_device(hidden, tok_perm, send_off, send_len, recv_off, recv_len, recv_doc, recv_pos, *params):
        n_tok = hidden.shape[0]
        n_cap = recv_doc.shape[0]
        n_dev = send_off.shape[0]
        at_start = jnp.arange(n_cap, dtype=jnp.int32)[None, :] == recv_off[:, None]
        start_pos = jnp.sum(jnp.where(at_start, recv_pos[None, :], 0), axis=1)
        broken = jnp.sum(jnp.where(recv_len > 0, start_pos, 0))
        mine = jnp.concatenate([recv_pos, send_len, recv_off, jnp.full((112,), broken, jnp.int32)])
        every = lax.all_gather(mine, 'sp', axis=0)
        pos_all = every[:, :n_cap]
        send_all = every[:, n_cap:n_cap + n_dev]
        roff_all = every[:, n_cap + n_dev:n_cap + 2 * n_dev]
        totals, starts, offs = ring_plan(send_all, n_cap)
        prev_totals = jnp.concatenate([totals[-1:], totals[:-1]])
        fits = jnp.all((offs >= -prev_totals) & (offs <= totals) & (jnp.abs(offs) <= n_cap))
        whole = jnp.sum(jnp.abs(every[:, n_cap + 2 * n_dev])) == 0
        use_ring = fits & whole

        me = lax.axis_index('sp').astype(jnp.int32)
        ring_at = jnp.where(me < 4, me, me ^ 2)
        after = lax.rem(ring_at + 1, n_dev)
        off = jnp.clip(offs[ring_at], -n_cap, n_cap)
        off_next = jnp.clip(offs[after], -n_cap, n_cap)
        total = totals[ring_at]
        spread = jnp.arange(2 * n_cap, dtype=jnp.int32)
        ext_idx = lax.dynamic_slice(jnp.concatenate([spread, tok_perm, spread]), (n_cap + off,), (3 * n_cap,))
        n_left = jnp.maximum(-off, 0)
        n_right = jnp.maximum(off_next, 0)
        reach = jnp.max(jnp.abs(offs))
        bucket = sum((reach > level).astype(jnp.int32) for level in LEVELS[:-1])

        order_of = ring_order(n_dev)
        runs = jnp.stack([send_all[d] for d in order_of])
        run_slot = jnp.stack([roff_all[:, d] for d in order_of])
        run_rel = starts[:, None] + jnp.cumsum(runs, axis=1) - runs - starts[ring_at] - off
        half = n_dev * n_cap // 2
        run_rel = jnp.where(run_rel >= half, run_rel - 2 * half, jnp.where(run_rel < -half, run_rel + 2 * half, run_rel))
        in_run = jnp.arange(n_cap, dtype=jnp.int32)[:, None] - run_rel.reshape(1, -1)
        run_base = (jnp.arange(n_dev, dtype=jnp.int32)[None, :] * every.shape[1] + run_slot).reshape(1, -1)
        from_at = jnp.sum(jnp.where((in_run >= 0) & (in_run < runs.reshape(1, -1)), run_base + in_run, 0), axis=1)
        plan = (ext_idx, from_at, every, off, total, n_left, n_right, bucket)

        def ring(_):
            return balanced_path(plan, hidden, tok_perm, *params)

        def general(_):
            return general_path(hidden, tok_perm, send_off, send_len, recv_off, recv_len, recv_doc, recv_pos, *params)

        return lax.cond(use_ring, ring, general, 0)

    return jax.shard_map(per_device, mesh=mesh, in_specs=(row_spec,) + (vec_spec,) * 7 + (rep_spec,) * 9, out_specs=row_spec, check_vma=False)
```
